256 devices in a mesh: dp: 128 (over z, x, y_hi, core), tensor: 2 (over y_lo).
Axes of the slice: x: 4, y: 4 (y_hi: 2, y_lo: 2; y = y_hi * 2 + y_lo), z: 8, core: 2. Of those that a mesh axis runs over, the one named last changes fastest.
Arguments:
- tokens: bfloat16 [16384, 2048], P('dp'), may hold values from -16 to 16
- teacher: bfloat16 [16384, 2048], P('dp'), may hold values from -6 to 6
- inner_weight: float32 [2048, 512], P('dp', 'tensor'), may hold values from -0.125 to 0.125
- output_weight: bfloat16 [2048, 2048], P('dp', 'tensor'), may hold values from -0.125 to 0.125
- inner_first: float32 [2048, 512], P('dp', 'tensor'), may hold values from -2 to 2
- inner_second: float32 [2048, 512], P('dp', 'tensor'), may hold values from 0.2 to 2
- state_weight: bfloat16 [2048, 32], replicated, may hold values from -0.03125 to 0.03125
- step_weight: bfloat16 [2048, 16], P(None, 'tensor'), may hold values from -0.0390625 to 0.0390625
- step_bias: float32 [16], P('tensor'), may hold values from -4 to 0
- decay_log: float32 [16], P('tensor'), may hold values from -3 to 1
- skip_gain: float32 [16], P('tensor'), may hold values from 0.5 to 1.5
Outputs:
- distill_loss: float32 [], replicated
- inner_update: float32 [2048, 512], P('dp', 'tensor')
- inner_first_next: float32 [2048, 512], P('dp', 'tensor')
- inner_second_next: float32 [2048, 512], P('dp', 'tensor')
The draws below stay inside these ranges and needn't reach their ends.
All inputs are finite; a program needn't handle non-finite values.
Results may differ from the reference program's by a relative error of at most 0.0016.
Values may be sent and summed in bfloat16 or wider, within the bound.
A program may use at most 64 MiB of HBM per device.

```python
import math
import jax
import jax.numpy as jnp
from jax import lax

D = 2048
HEADS = 16
GROUPS = 4
HEAD_DIM = 128
STATE = 16
TOK_DEV = 128
STEP = 20
INNER = 2048
XB = 512
TOKENS = 16384
N_DP = 128


def draw_tokens(key, part):
    key_base, key_cols = jax.random.split(key, 2)
    base = jax.random.normal(key_base, (TOKENS, D), jnp.float32)
    column = jnp.arange(D, dtype=jnp.float32) / D
    spread = jnp.exp(jax.random.uniform(key_cols, (D,), jnp.float32, 0.0, jnp.log(2.0)))
    rising = jnp.exp(jnp.log(3.0) * column) * spread
    values = base * rising[None, :] / 2.0
    return jnp.clip(values, -16.0, 16.0).astype(jnp.bfloat16)


def levels(rng, extent, cuts, least, largest):
    def one(axis_at, shards_of):
        draws = jax.random.uniform(jax.random.fold_in(jax.random.fold_in(rng, 6), axis_at), (shards_of,), jnp.float32, least / len(cuts), largest / len(cuts))
        return jnp.repeat(jnp.exp(draws), extent[axis_at] // shards_of).reshape((-1,) + (1,) * (len(extent) - axis_at - 1))

    level = one(*cuts[0])
    for cut in cuts[1:]:
        level = level * one(*cut)
    return level


def normal_values(stream_key, shape, scale, limit, cuts=(), kind=jnp.bfloat16):
    drawn = jax.random.normal(stream_key, shape, jnp.float32) * scale
    if len(cuts) > 0:
        drawn = levels(stream_key, shape, cuts, -0.22, 0.18) * drawn
    return jnp.clip(drawn, min=-limit, max=limit).astype(kind)


def setup_inputs(seed: int = 0) -> dict:
    key_list = jax.random.split(jax.random.key(seed), 12)
    return {
        "tokens": draw_tokens(jax.random.fold_in(key_list[11], 71), 0),
        "teacher": normal_values(key_list[1], (TOKENS, D), 1.0, 6.0, ((0, 128),)),
        "inner_weight": normal_values(key_list[2], (D, XB), D ** -0.5, 0.125, ((0, 128), (1, 2)), jnp.float32),
        "output_weight": normal_values(key_list[3], (D, INNER), INNER ** -0.5, 0.125, ((0, 128), (1, 2))),
        "inner_first": normal_values(key_list[4], (D, XB), 0.3, 2.0, ((0, 128), (1, 2)), jnp.float32),
        "inner_second": jnp.clip(jnp.exp(math.log(2.0) - 2.3025851 * jax.random.uniform(key_list[5], (D, XB), jnp.float32) ** levels(key_list[5], (D, XB), ((0, 128), (1, 2)), -0.2, 0.2)), 0.2, 2.0),
        "state_weight": normal_values(key_list[6], (D, 2 * STATE), (D * STATE) ** -0.5, 0.03125),
        "step_weight": normal_values(key_list[7], (D, HEADS), (10 * D) ** -0.5, 0.0390625, ((1, 2),)),
        "step_bias": jnp.clip(-4.0 + 4.0 * jax.random.uniform(key_list[8], (HEADS,), jnp.float32) ** levels(key_list[8], (HEADS,), ((0, 2),), -0.2, 0.2), -4.0, 0.0),
        "decay_log": jnp.clip(-3.0 + 4.0 * jax.random.uniform(key_list[9], (HEADS,), jnp.float32) ** levels(key_list[9], (HEADS,), ((0, 2),), -0.2, 0.2), -3.0, 1.0),
        "skip_gain": jnp.clip(0.5 + 1.0 * jax.random.uniform(key_list[10], (HEADS,), jnp.float32) ** levels(key_list[10], (HEADS,), ((0, 2),), -0.2, 0.2), 0.5, 1.5),
    }


beta_one = 0.9
beta_two = 0.95
adam_eps = 1e-08
weight_decay = 0.1
norm_eps = 1e-06

def mixing(sequence, state_weight, step_weight, step_bias, decay_log):
    state_width = state_weight.shape[1] // 2
    projected = jnp.dot(sequence, state_weight, preferred_element_type=jnp.float32)
    b_coef = projected[:, :state_width]
    c_coef = projected[:, state_width:]
    gram_matrix = jnp.dot(c_coef, b_coef.T, precision=lax.Precision.HIGHEST)
    step_size = jax.nn.softplus(jnp.dot(sequence, step_weight, preferred_element_type=jnp.float32) + step_bias)
    rate_step = jnp.exp(decay_log) * step_size
    cumulative = jnp.cumsum(rate_step, axis=0).T
    length = sequence.shape[0]
    row_later = lax.broadcasted_iota(jnp.int32, (length, length), 0)
    earlier = lax.broadcasted_iota(jnp.int32, (length, length), 1)
    causal = row_later >= earlier
    log_decay = cumulative[:, None, :] - cumulative[:, :, None]
    decay_matrix = jnp.where(causal[None], jnp.exp(jnp.minimum(log_decay, 0.0)), 0.0)
    return (gram_matrix[None] * decay_matrix * step_size.T[:, None, :]).astype(jnp.bfloat16)

def reference(tokens, teacher, inner_weight, output_weight, inner_first, inner_second, state_weight, step_weight, step_bias, decay_log, skip_gain):
    inner_half = inner_weight.astype(jnp.bfloat16)
    ratio = HEADS // GROUPS
    sequences = tokens.reshape(N_DP, TOK_DEV, D)
    targets = teacher.reshape(N_DP, TOK_DEV, D)

    def one_sequence(running, inputs_pair):
        sequence, target = inputs_pair
        weights_mix = mixing(sequence, state_weight, step_weight, step_bias, decay_log).astype(jnp.float32)
        projected = jnp.dot(sequence, inner_half, preferred_element_type=jnp.float32).astype(jnp.bfloat16)
        groups_in = projected.reshape(TOK_DEV, GROUPS, HEAD_DIM).astype(jnp.float32)
        heads_in = jnp.repeat(groups_in, ratio, axis=1)
        mixed = jnp.einsum('hts,shp->thp', weights_mix, heads_in) + skip_gain[None, :, None] * heads_in
        inner = mixed.astype(jnp.bfloat16).reshape(TOK_DEV, INNER)
        student = lax.dot_general(inner, output_weight, (((1,), (1,)), ((), ())), preferred_element_type=jnp.float32)
        error_rows = student - target.astype(jnp.float32)
        grad_out = error_rows.astype(jnp.bfloat16)
        grad_inner = jnp.dot(grad_out, output_weight, preferred_element_type=jnp.float32).astype(jnp.bfloat16)
        grad_heads = grad_inner.reshape(TOK_DEV, HEADS, HEAD_DIM).astype(jnp.float32)
        back = jnp.einsum('hts,thp->shp', weights_mix, grad_heads) + skip_gain[None, :, None] * grad_heads
        grouped = lax.optimization_barrier(jnp.sum(back.reshape(TOK_DEV, GROUPS, ratio, HEAD_DIM), axis=2))
        grad_projected = grouped.astype(jnp.bfloat16).reshape(TOK_DEV, XB)
        inner_term = jnp.dot(sequence.T, grad_projected, preferred_element_type=jnp.float32)
        return ((running[0] + inner_term, running[1] + jnp.sum(error_rows * error_rows)), None)
    initial = (jnp.zeros((D, XB), jnp.float32), jnp.zeros((), jnp.float32))
    (inner_grad, square_sum), _ = lax.scan(one_sequence, initial, (sequences, targets))
    distill_loss = square_sum / (TOKENS * D)
    root_mean = jnp.sqrt(jnp.sum(inner_grad * inner_grad) / (D * XB))
    factor = jnp.minimum(1.0, 1.0 / (root_mean + norm_eps))
    first_fix = 1.0 - beta_one ** STEP
    second_fix = 1.0 - beta_two ** STEP
    clipped = factor * inner_grad
    first_next = beta_one * inner_first + (1.0 - beta_one) * clipped
    second_next = beta_two * inner_second + (1.0 - beta_two) * clipped * clipped
    update = first_next / first_fix / (jnp.sqrt(second_next / second_fix) + adam_eps) + weight_decay * inner_weight
    return (distill_loss, update, first_next, second_next)
```

```python
import functools
import heapq

import jax
import jax.numpy as jnp
from jax import lax
from jax.experimental import pallas as pl
from jax.experimental.pallas import tpu as pltpu
from jax.sharding import Mesh
from jax.sharding import PartitionSpec as P

HEADS = 16
GROUPS = 4
HEAD_DIM = 128
STEP = 20
DP = ("dp_0", "dp_1", "dp_2", "dp_3")
DP_TENSOR = ("dp_0", "dp_1", "dp_2", "dp_3", "tensor")


beta_one = 0.9
beta_two = 0.95
adam_eps = 1e-08
weight_decay = 0.1
norm_eps = 1e-06


SIZES = {"dp_0": 8, "dp_1": 4, "dp_2": 2}


def relay_plan(order, sizes, wire=0.88, latency=1.8):
    def direction(rel, k):
        n, v = sizes[order[k]], rel[k]
        if n == 2:
            return 1
        if 2 * v == n:
            return 1 if sum(rel[:k]) % 2 == 0 else -1
        return 1 if 2 * v < n else -1

    def children(rel):
        last = max([k for k in range(3) if rel[k]], default=-1)
        out = []
        if last >= 0 and sizes[order[last]] > 2:
            sign = direction(rel, last)
            n = sizes[order[last]]
            nxt = list(rel)
            nxt[last] = (rel[last] + sign) % n
            steps_now = rel[last] if sign > 0 else n - rel[last]
            steps_nxt = nxt[last] if sign > 0 else n - nxt[last]
            if nxt[last] and steps_nxt == steps_now + 1 and direction(nxt, last) == sign:
                out.append((last, sign, tuple(nxt)))
        for k in range(last + 1, 3):
            n = sizes[order[k]]
            for sign in (1, -1) if n > 2 else (1,):
                nxt = list(rel)
                nxt[k] = sign % n
                out.append((k, sign, tuple(nxt)))
        return out

    root = (0, 0, 0)
    free = {}
    ready = [(0.0, root)]
    steps = []
    while ready:
        now, rel = heapq.heappop(ready)
        sends = children(rel)
        steps.append((now, rel, sends))
        for k, sign, nxt in sends:
            begin = max(now, free.get((k, sign), 0.0))
            free[(k, sign)] = begin + wire
            heapq.heappush(ready, (begin + wire + latency + (0.8 if sizes[order[k]] == 2 else 0), nxt))
    return steps


TORUS = ("dp_0", "dp_1", "dp_2")
ORDERS = (("dp_2", "dp_1", "dp_0"), ("dp_2", "dp_0", "dp_1"))


def enter_with(peers):
    barrier = pltpu.get_barrier_semaphore()
    for peer in peers:
        pl.semaphore_signal(barrier, inc=1, device_id=peer, device_id_type=pl.DeviceIdType.MESH)
    pl.semaphore_wait(barrier, len(peers))


def gather_kernel(sizes, mine, out, send_sem, recv_sem, pair_sem):
    here = {a: lax.axis_index(a) for a in TORUS}
    core = lax.axis_index("dp_3")

    def shifted(axis, by):
        return lax.rem(here[axis] + (by % sizes[axis]), sizes[axis])

    other = {"dp_3": 1 - core}
    neighbours = [{a: shifted(a, s)} for a in TORUS for s in ((1, -1) if sizes[a] > 2 else (1,))]
    enter_with(neighbours + [other])

    def relay(order, core_id):
        def slot(rel):
            at = {a: shifted(a, -v) for a, v in zip(order, rel)}
            return ((at["dp_0"] * sizes["dp_1"] + at["dp_1"]) * sizes["dp_2"] + at["dp_2"]) * 2 + core_id

        def number(rel):
            return (rel[0] * sizes[order[1]] + rel[1]) * sizes[order[2]] + rel[2]

        for _, rel, sends in relay_plan(order, sizes):
            own = not any(rel)
            where = slot(rel)
            block = mine if own else out.at[where]
            if not own:
                pltpu.make_async_remote_copy(
                    out.at[where], out.at[where], send_sem, recv_sem.at[number(rel)],
                    device_id=other, device_id_type=pl.DeviceIdType.MESH,
                ).wait_recv()
            for k, sign, nxt in sends:
                pltpu.make_async_remote_copy(
                    block, out.at[where], send_sem, recv_sem.at[number(nxt)],
                    device_id={order[k]: shifted(order[k], sign)},
                    device_id_type=pl.DeviceIdType.MESH,
                ).start()
            pltpu.make_async_remote_copy(
                block, out.at[where], send_sem, pair_sem,
                device_id=other, device_id_type=pl.DeviceIdType.MESH,
            ).start()
            if own:
                out[where] = mine[...]

    @pl.when(core == 0)
    def _():
        relay(ORDERS[0], 0)

    @pl.when(core == 1)
    def _():
        relay(ORDERS[1], 1)

    pieces = sizes["dp_0"] * sizes["dp_1"] * sizes["dp_2"]
    pltpu.make_async_remote_copy(
        out.at[pl.ds(0, pieces)], out.at[pl.ds(0, pieces)], send_sem, pair_sem,
        device_id=other, device_id_type=pl.DeviceIdType.MESH,
    ).wait_recv()
    sent = 2 * pieces - 1
    pltpu.make_async_remote_copy(
        out.at[pl.ds(0, sent)], out.at[pl.ds(0, sent)], send_sem, pair_sem,
        device_id=other, device_id_type=pl.DeviceIdType.MESH,
    ).wait_send()


def gathered(mine):
    sizes = {a: lax.axis_size(a) for a in TORUS}
    pieces = sizes["dp_0"] * sizes["dp_1"] * sizes["dp_2"]
    return pl.pallas_call(
        functools.partial(gather_kernel, sizes),
        name="gather",
        out_shape=jax.ShapeDtypeStruct((2 * pieces, *mine.shape), mine.dtype),
        in_specs=[pl.BlockSpec(memory_space=pltpu.VMEM)],
        out_specs=pl.BlockSpec(memory_space=pltpu.VMEM),
        scratch_shapes=[
            pltpu.SemaphoreType.DMA,
            pltpu.SemaphoreType.DMA((pieces,)),
            pltpu.SemaphoreType.DMA,
        ],
        compiler_params=pltpu.CompilerParams(
            collective_id=0, has_side_effects=True, vmem_limit_bytes=16 * 1024 * 1024
        ),
    )(mine)


def sent_to_all(x, axis):
    peers = lax.axis_size(axis)
    return lax.all_to_all(jnp.broadcast_to(x[None], (peers, *x.shape)), axis, 0, 0, tiled=True)


def of_everyone(x, axis):
    everything = sent_to_all(x, axis)
    return jnp.sum(everything, axis=0)


def cut_along(x, dim, peers):
    before, after = (x.shape[:dim], x.shape[dim + 1 :])
    return jnp.moveaxis(x.reshape(*before, peers, -1, *after), dim, 0)


def sum_at_owner(x, axis, dim):
    peers = lax.axis_size(axis)
    pieces = lax.all_to_all(cut_along(x, dim, peers), axis, 0, 0, tiled=True)
    return jnp.sum(pieces, axis=0)


def sum_in_two_steps(x, axes, dim):
    far, near = axes
    own = sum_at_owner(cut_along(x, dim, lax.axis_size(far)), near, dim + 1)
    return jnp.sum(lax.all_to_all(own, far, 0, 0, tiled=True), axis=0)


def mixing(sequence, state_weight, step_weight, step_bias, decay_log):
    state_width = state_weight.shape[1] // 2
    projected = jnp.dot(sequence, state_weight, preferred_element_type=jnp.float32)
    b_coef = projected[:, :state_width]
    c_coef = projected[:, state_width:]
    gram_matrix = jnp.dot(c_coef, b_coef.T, precision=lax.Precision.HIGHEST)
    step_size = jax.nn.softplus(
        jnp.dot(sequence, step_weight, preferred_element_type=jnp.float32) + step_bias
    )
    rate_step = jnp.exp(decay_log) * step_size
    cumulative = jnp.cumsum(rate_step, axis=0).T
    length = sequence.shape[0]
    row_later = lax.broadcasted_iota(jnp.int32, (length, length), 0)
    earlier = lax.broadcasted_iota(jnp.int32, (length, length), 1)
    causal = row_later >= earlier
    log_decay = cumulative[:, None, :] - cumulative[:, :, None]
    decay_matrix = jnp.where(causal[None], jnp.exp(jnp.minimum(log_decay, 0.0)), 0.0)
    return (gram_matrix[None] * decay_matrix * step_size.T[:, None, :]).astype(jnp.bfloat16)


def contract_rows(left, right):
    return lax.dot_general(
        left, right, (((0,), (0,)), ((), ())), preferred_element_type=jnp.float32
    )


def on_device(
    tokens,
    teacher,
    inner_weight,
    output_weight,
    inner_first,
    inner_second,
    state_weight,
    step_weight,
    step_bias,
    decay_log,
    skip_gain,
):
    seq_rows, model_width = tokens.shape
    heads_here = step_weight.shape[1]
    groups_here = inner_weight.shape[1] // HEAD_DIM
    ratio = HEADS // GROUPS
    total_tokens = seq_rows * lax.axis_size(DP)
    whole = gathered(jnp.concatenate([inner_weight.astype(jnp.bfloat16), output_weight], axis=1))
    whole = whole.reshape(model_width, whole.shape[-1])
    inner_full, output_full = jnp.split(whole, [inner_weight.shape[1]], axis=1)
    weights_mix = mixing(tokens, state_weight, step_weight, step_bias, decay_log)
    projected = jnp.dot(tokens, inner_full, preferred_element_type=jnp.float32).astype(jnp.bfloat16)
    heads_in = jnp.repeat(projected.reshape(seq_rows, groups_here, HEAD_DIM), ratio, axis=1)
    mixed = jnp.einsum(
        "hts,shp->thp", weights_mix, heads_in, preferred_element_type=jnp.float32
    ) + skip_gain[None, :, None] * heads_in.astype(jnp.float32)
    inner = mixed.astype(jnp.bfloat16).reshape(seq_rows, heads_here * HEAD_DIM)
    partial_out = lax.dot_general(
        inner, output_full, (((1,), (1,)), ((), ())), preferred_element_type=jnp.float32
    )
    student = of_everyone(partial_out, "tensor")
    error_rows = student - teacher.astype(jnp.float32)
    square_sum = jnp.where(lax.axis_index("tensor") == 0, jnp.sum(error_rows * error_rows), 0.0)
    grad_out = error_rows.astype(jnp.bfloat16)
    grad_inner = jnp.dot(grad_out, output_full, preferred_element_type=jnp.float32).astype(
        jnp.bfloat16
    )
    grad_heads = grad_inner.reshape(seq_rows, heads_here, HEAD_DIM)
    back = jnp.einsum(
        "hts,thp->shp", weights_mix, grad_heads, preferred_element_type=jnp.float32
    ) + skip_gain[None, :, None] * grad_heads.astype(jnp.float32)
    grouped = jnp.sum(back.reshape(seq_rows, groups_here, ratio, HEAD_DIM), axis=2)
    grad_projected = grouped.astype(jnp.bfloat16).reshape(seq_rows, groups_here * HEAD_DIM)
    inner_grad = sum_in_two_steps(
        contract_rows(tokens, grad_projected), (("dp_0", "dp_1", "dp_2"), "dp_3"), 0
    )
    local_squares = jnp.sum(inner_grad * inner_grad)
    squares_total, error_total = lax.psum(jnp.stack([local_squares, square_sum]), DP_TENSOR)
    entry_count = model_width * groups_here * HEAD_DIM * lax.axis_size("tensor")
    root_mean = jnp.sqrt(squares_total / entry_count)
    factor = jnp.minimum(1.0, 1.0 / (root_mean + norm_eps))
    distill_loss = error_total / (total_tokens * model_width)
    first_fix = 1.0 - beta_one**STEP
    second_fix = 1.0 - beta_two**STEP
    clipped = factor * inner_grad
    first_next = beta_one * inner_first + (1.0 - beta_one) * clipped
    second_next = beta_two * inner_second + (1.0 - beta_two) * clipped * clipped
    update = (
        first_next / first_fix / (jnp.sqrt(second_next / second_fix) + adam_eps)
        + weight_decay * inner_weight
    )
    return (distill_loss, update, first_next, second_next)


def solution(mesh):
    finer = Mesh(
        mesh.devices.reshape(8, 4, 2, 2, mesh.shape["tensor"]),
        ("dp_0", "dp_1", "dp_2", "dp_3", "tensor"),
    )
    return jax.shard_map(
        on_device,
        mesh=finer,
        in_specs=(
            P(DP, None),
            P(DP, None),
            P(DP, "tensor"),
            P(DP, "tensor"),
            P(DP, "tensor"),
            P(DP, "tensor"),
            P(),
            P(None, "tensor"),
            P("tensor"),
            P("tensor"),
            P("tensor"),
        ),
        out_specs=(P(), P(DP, "tensor"), P(DP, "tensor"), P(DP, "tensor")),
        check_vma=False,
    )
```

```python
import functools
import heapq

import jax
import jax.numpy as jnp
from jax import lax
from jax.experimental import pallas as pl
from jax.experimental.pallas import tpu as pltpu
from jax.sharding import Mesh
from jax.sharding import PartitionSpec as P

HEADS = 16
GROUPS = 4
HEAD_DIM = 128
STEP = 20
DP = ("dp_0", "dp_1", "dp_2", "dp_3")
DP_TENSOR = ("dp_0", "dp_1", "dp_2", "dp_3", "tensor")


beta_one = 0.9
beta_two = 0.95
adam_eps = 1e-08
weight_decay = 0.1
norm_eps = 1e-06


SIZES = {"dp_0": 8, "dp_1": 4, "dp_2": 2}


def relay_plan(order, sizes, wire=0.88, latency=1.8):
    def direction(rel, k):
        n, v = sizes[order[k]], rel[k]
        if n == 2:
            return 1
        if 2 * v == n:
            return 1 if sum(rel[:k]) % 2 == 0 else -1
        return 1 if 2 * v < n else -1

    def children(rel):
        last = max([k for k in range(3) if rel[k]], default=-1)
        out = []
        if last >= 0 and sizes[order[last]] > 2:
            sign = direction(rel, last)
            n = sizes[order[last]]
            nxt = list(rel)
            nxt[last] = (rel[last] + sign) % n
            steps_now = rel[last] if sign > 0 else n - rel[last]
            steps_nxt = nxt[last] if sign > 0 else n - nxt[last]
            if nxt[last] and steps_nxt == steps_now + 1 and direction(nxt, last) == sign:
                out.append((last, sign, tuple(nxt)))
        for k in range(last + 1, 3):
            n = sizes[order[k]]
            for sign in (1, -1) if n > 2 else (1,):
                nxt = list(rel)
                nxt[k] = sign % n
                out.append((k, sign, tuple(nxt)))
        return out

    root = (0, 0, 0)
    free = {}
    ready = [(0.0, root)]
    steps = []
    while ready:
        now, rel = heapq.heappop(ready)
        sends = children(rel)
        steps.append((now, rel, sends))
        for k, sign, nxt in sends:
            begin = max(now, free.get((k, sign), 0.0))
            free[(k, sign)] = begin + wire
            heapq.heappush(ready, (begin + wire + latency + (0.8 if sizes[order[k]] == 2 else 0), nxt))
    return steps


TORUS = ("dp_0", "dp_1", "dp_2")
ORDERS = (("dp_2", "dp_1", "dp_0"), ("dp_2", "dp_0", "dp_1"))


def enter_with(peers):
    barrier = pltpu.get_barrier_semaphore()
    for peer in peers:
        pl.semaphore_signal(barrier, inc=1, device_id=peer, device_id_type=pl.DeviceIdType.MESH)
    pl.semaphore_wait(barrier, len(peers))


def gather_kernel(sizes, mine, out, send_sem, recv_sem, pair_sem):
    here = {a: lax.axis_index(a) for a in TORUS}
    core = lax.axis_index("dp_3")

    def shifted(axis, by):
        return lax.rem(here[axis] + (by % sizes[axis]), sizes[axis])

    other = {"dp_3": 1 - core}
    neighbours = [{a: shifted(a, s)} for a in TORUS for s in ((1, -1) if sizes[a] > 2 else (1,))]
    enter_with(neighbours + [other])

    def relay(order, core_id):
        def slot(rel):
            at = {a: shifted(a, -v) for a, v in zip(order, rel)}
            return ((at["dp_0"] * sizes["dp_1"] + at["dp_1"]) * sizes["dp_2"] + at["dp_2"]) * 2 + core_id

        def number(rel):
            return (rel[0] * sizes[order[1]] + rel[1]) * sizes[order[2]] + rel[2]

        for _, rel, sends in relay_plan(order, sizes):
            own = not any(rel)
            where = slot(rel)
            block = mine if own else out.at[where]
            if not own:
                pltpu.make_async_remote_copy(
                    out.at[where], out.at[where], send_sem, recv_sem.at[number(rel)],
                    device_id=other, device_id_type=pl.DeviceIdType.MESH,
                ).wait_recv()
            for k, sign, nxt in sends:
                pltpu.make_async_remote_copy(
                    block, out.at[where], send_sem, recv_sem.at[number(nxt)],
                    device_id={order[k]: shifted(order[k], sign)},
                    device_id_type=pl.DeviceIdType.MESH,
                ).start()
            pltpu.make_async_remote_copy(
                block, out.at[where], send_sem, pair_sem,
                device_id=other, device_id_type=pl.DeviceIdType.MESH,
            ).start()
            if own:
                out[where] = mine[...]

    @pl.when(core == 0)
    def _():
        relay(ORDERS[0], 0)

    @pl.when(core == 1)
    def _():
        relay(ORDERS[1], 1)

    pieces = sizes["dp_0"] * sizes["dp_1"] * sizes["dp_2"]
    pltpu.make_async_remote_copy(
        out.at[pl.ds(0, pieces)], out.at[pl.ds(0, pieces)], send_sem, pair_sem,
        device_id=other, device_id_type=pl.DeviceIdType.MESH,
    ).wait_recv()
    sent = 2 * pieces - 1
    pltpu.make_async_remote_copy(
        out.at[pl.ds(0, sent)], out.at[pl.ds(0, sent)], send_sem, pair_sem,
        device_id=other, device_id_type=pl.DeviceIdType.MESH,
    ).wait_send()


def gathered(mine):
    sizes = {a: lax.axis_size(a) for a in TORUS}
    pieces = sizes["dp_0"] * sizes["dp_1"] * sizes["dp_2"]
    return pl.pallas_call(
        functools.partial(gather_kernel, sizes),
        name="gather",
        out_shape=jax.ShapeDtypeStruct((2 * pieces, *mine.shape), mine.dtype),
        in_specs=[pl.BlockSpec(memory_space=pltpu.VMEM)],
        out_specs=pl.BlockSpec(memory_space=pltpu.VMEM),
        scratch_shapes=[
            pltpu.SemaphoreType.DMA,
            pltpu.SemaphoreType.DMA((pieces,)),
            pltpu.SemaphoreType.DMA,
        ],
        compiler_params=pltpu.CompilerParams(
            collective_id=0, has_side_effects=True, vmem_limit_bytes=16 * 1024 * 1024
        ),
    )(mine)


CHUNK = 256


def step_kernel(
    sizes, inner, weight, tokens, teacher, mix, skip, grad_out, sums_out,
    tok_t, tok_all, mix_t, part, leaving, arrived, grad_acc, gp_all, g_part, g_all, row_a, row_b,
    student_send, student_recv, tok_send, tok_recv, gp_send, gp_recv,
    g_send, g_recv, a_send, a_recv, b_send, b_recv,
):
    axes = ("dp_0", "dp_1", "dp_2", "dp_3", "tensor")
    here = {a: lax.axis_index(a) for a in axes}
    nz, nx, ny = sizes["dp_0"], sizes["dp_1"], sizes["dp_2"]
    features, cols = weight.shape
    chunks = features // CHUNK
    head_dim = mix.shape[-1]
    groups = gp_all.shape[-1] // head_dim
    per_group = cols // head_dim // groups

    def there(**by):
        return {
            a: lax.rem(here[a] + v, sizes[a]) for a, v in by.items() if v % sizes[a]
        }

    def remote(src, dst, send, recv, target):
        return pltpu.make_async_remote_copy(
            src, dst, send, recv, device_id=target, device_id_type=pl.DeviceIdType.MESH
        )

    plane = [
        dict(dp_1=i, dp_2=j, dp_3=k, tensor=t)
        for i in range(nx) for j in range(ny) for k in range(2) for t in range(2)
    ][1:]
    column = [dict(dp_0=i, dp_2=j) for i in range(nz) for j in range(ny)][1:]
    peers = plane + [by for by in column if by["dp_0"]]
    barrier = pltpu.get_barrier_semaphore()
    for by in peers:
        pl.semaphore_signal(
            barrier, inc=1, device_id=there(**by), device_id_type=pl.DeviceIdType.MESH
        )

    other_half = there(tensor=1)

    def student_copy(i):
        return remote(
            leaving.at[i], arrived.at[i], student_send, student_recv.at[i], other_half
        )

    for i in range(chunks):
        rows = weight[pl.ds(i * CHUNK, CHUNK), :]
        piece = lax.dot_general(
            inner[...], rows, (((1,), (1,)), ((), ())), preferred_element_type=jnp.float32
        )
        part[i] = piece
        leaving[i] = piece.astype(jnp.bfloat16)
        if i == 0:
            pl.semaphore_wait(barrier, len(peers))
        else:
            student_copy(i - 1).start()
    student_copy(chunks - 1).start()

    seq = tokens.shape[0]
    for k in range(features // 128):
        turned = tokens[:, k * 128 : (k + 1) * 128].T
        per = tok_t.shape[4]
        tok_t[k * 128 // (nx * ny * 2 * per), (k * 128 // (ny * 2 * per)) % nx : (k * 128 // (ny * 2 * per)) % nx + 128 // (ny * 2 * per)] = (
            turned.reshape(128 // (ny * 2 * per), ny, 2, per, seq)
        )
    tok_sends = []
    for i in range(nx):
        for k in range(2):
            slot = i * 2 + k
            to_x = lax.rem(here["dp_1"] + i, nx)
            to_c = lax.rem(here["dp_3"] + k, 2)
            if slot:
                tok_sends.append((slot, to_x, to_c, there(dp_1=i, dp_3=k)))
    for slot, to_x, to_c, target in tok_sends:
        remote(
            tok_t.at[:, to_x, :, to_c], tok_all.at[slot], tok_send, tok_recv, target
        ).start()
    tok_all[0] = tok_t[:, here["dp_1"], :, here["dp_3"]]
    for g in range(groups):
        for h in range(per_group):
            mix_t[g, :, h * seq : (h + 1) * seq] = mix[g * per_group + h].T

    squares = jnp.zeros((8, CHUNK), jnp.float32)
    for i in range(chunks):
        student_copy(i).wait_recv()
        error = (
            part[i] + arrived[i].astype(jnp.float32)
            - teacher[:, i * CHUNK : (i + 1) * CHUNK].astype(jnp.float32)
        )
        squares = squares + jnp.sum((error * error).reshape(seq // 8, 8, CHUNK), axis=0)
        product = jnp.dot(
            error.astype(jnp.bfloat16), weight[pl.ds(i * CHUNK, CHUNK), :],
            preferred_element_type=jnp.float32,
        )
        if i == 0:
            grad_acc[...] = product
        else:
            grad_acc[...] += product
    for g in range(groups):
        heads = []
        direct = None
        for h in range(per_group):
            at = slice((g * per_group + h) * head_dim, (g * per_group + h + 1) * head_dim)
            one = grad_acc[:, at].astype(jnp.bfloat16)
            heads.append(one)
            term = skip[:, at] * one.astype(jnp.float32)
            direct = term if direct is None else direct + term
        back = jnp.dot(
            mix_t[g], jnp.concatenate(heads, axis=0), preferred_element_type=jnp.float32
        )
        gp_all[0, :, g * head_dim : (g + 1) * head_dim] = (back + direct).astype(jnp.bfloat16)

    pair = there(dp_3=1)
    for i in (2, 1, 3) if nx == 4 else range(1, nx):
        remote(
            gp_all.at[0], gp_all.at[2 * i], gp_send, gp_recv.at[2 * i], there(dp_1=i)
        ).start()
    remote(gp_all.at[0], gp_all.at[1], gp_send, gp_recv.at[1], pair).start()
    members = 2 * nx
    block = tok_all.at[0]
    remote(
        tok_all.at[pl.ds(1, members - 1)], tok_all.at[pl.ds(1, members - 1)],
        tok_send, tok_recv, pair,
    ).wait()

    def product_of(slot):
        left = tok_all[slot].reshape(-1, seq)
        return jnp.dot(left, gp_all[slot], preferred_element_type=jnp.float32)

    remote(gp_all.at[1], gp_all.at[1], gp_send, gp_recv.at[1], pair).wait_recv()
    total = product_of(0) + product_of(1)
    order = (1, 3, 2) if nx == 4 else range(1, nx)
    for i in order:
        remote(gp_all.at[0], gp_all.at[2 * i], gp_send, gp_recv.at[2 * i], pair).wait_recv()
        remote(
            gp_all.at[2 * i], gp_all.at[2 * i + 1], gp_send, gp_recv.at[2 * i + 1], pair
        ).start()
        total = total + product_of(2 * i)
    for i in order:
        remote(
            gp_all.at[0], gp_all.at[2 * i + 1], gp_send, gp_recv.at[2 * i + 1], pair
        ).wait_recv()
        total = total + product_of(2 * i + 1)
    g_part[...] = total.reshape(g_part.shape)

    for by in sorted(column, key=lambda b: -min(b["dp_0"], nz - b["dp_0"]) - b["dp_2"]):
        slot = by["dp_0"] * ny + by["dp_2"]
        to_z = lax.rem(here["dp_0"] + by["dp_0"], nz)
        to_y = lax.rem(here["dp_2"] + by["dp_2"], ny)
        remote(g_part.at[to_z, to_y], g_all.at[slot], g_send, g_recv, there(**by)).start()
    g_all[0] = g_part[here["dp_0"], here["dp_2"]]
    err = jnp.sum(squares) * 0.5
    rest = g_all.at[pl.ds(1, nz * ny - 1)]
    remote(rest, rest, g_send, g_recv, pair).wait()
    grad = jnp.sum(g_all[...], axis=0)
    grad_out[...] = grad
    lane = lax.broadcasted_iota(jnp.int32, (1, 128), 1)
    row = jnp.where(lane == 0, jnp.sum(grad * grad), jnp.where(lane == 1, err, 0.0))
    row_a[0] = row
    for n, by in enumerate(plane):
        remote(row_a.at[0], row_a.at[n + 1], a_send, a_recv, there(**by)).start()
    rest = row_a.at[pl.ds(1, len(plane))]
    remote(rest, rest, a_send, a_recv, pair).wait()
    row_b[0] = jnp.sum(row_a[...], axis=0)
    for i in range(1, nz):
        remote(row_b.at[0], row_b.at[i], b_send, b_recv, there(dp_0=i)).start()
    rest = row_b.at[pl.ds(1, nz - 1)]
    remote(rest, rest, b_send, b_recv, pair).wait()
    sums_out[...] = jnp.sum(row_b[...], axis=0)

    rest = gp_all.at[pl.ds(1, members - 1)]
    remote(rest, rest, gp_send, gp_recv.at[1], pair).wait_send()
    remote(leaving, leaving, student_send, student_recv.at[0], pair).wait_send()


def after_gather(inner, weight, tokens, teacher, mix, skip, own_rows):
    sizes = {a: lax.axis_size(a) for a in ("dp_0", "dp_1", "dp_2", "dp_3", "tensor")}
    nz, nx, ny = sizes["dp_0"], sizes["dp_1"], sizes["dp_2"]
    seq, features = tokens.shape
    cols = weight.shape[1]
    chunks = features // CHUNK
    heads = mix.shape[0]
    gcols = GROUPS // sizes["tensor"] * HEAD_DIM
    f32, half = jnp.float32, jnp.bfloat16
    vmem = pl.BlockSpec(memory_space=pltpu.VMEM)
    dma = pltpu.SemaphoreType.DMA
    return pl.pallas_call(
        functools.partial(step_kernel, sizes),
        name="after_gather",
        out_shape=(
            jax.ShapeDtypeStruct((own_rows, gcols), f32),
            jax.ShapeDtypeStruct((1, 128), f32),
        ),
        in_specs=[vmem] * 6,
        out_specs=(vmem, vmem),
        scratch_shapes=[
            pltpu.VMEM((nz, nx, ny, 2, own_rows, seq), half),
            pltpu.VMEM((2 * nx, nz, ny, own_rows, seq), half),
            pltpu.VMEM((gcols // HEAD_DIM, seq, heads * HEAD_DIM * seq // gcols), half),
            pltpu.VMEM((chunks, seq, CHUNK), f32),
            pltpu.VMEM((chunks, seq, CHUNK), half),
            pltpu.VMEM((chunks, seq, CHUNK), half),
            pltpu.VMEM((seq, cols), f32),
            pltpu.VMEM((2 * nx, seq, gcols), half),
            pltpu.VMEM((nz, ny, own_rows, gcols), f32),
            pltpu.VMEM((nz * ny, own_rows, gcols), f32),
            pltpu.VMEM((nx * ny * 4, 1, 128), f32),
            pltpu.VMEM((nz, 1, 128), f32),
            dma, dma((chunks,)), dma, dma, dma, dma((2 * nx,)),
            dma, dma, dma, dma, dma, dma,
        ],
        compiler_params=pltpu.CompilerParams(
            collective_id=1, has_side_effects=True, vmem_limit_bytes=32 * 1024 * 1024
        ),
    )(inner, weight, tokens, teacher, mix, skip)


def mixing(sequence, state_weight, step_weight, step_bias, decay_log):
    state_width = state_weight.shape[1] // 2
    projected = jnp.dot(sequence, state_weight, preferred_element_type=jnp.float32)
    b_coef = projected[:, :state_width]
    c_coef = projected[:, state_width:]
    gram_matrix = jnp.dot(c_coef, b_coef.T, precision=lax.Precision.HIGHEST)
    step_size = jax.nn.softplus(
        jnp.dot(sequence, step_weight, preferred_element_type=jnp.float32) + step_bias
    )
    rate_step = jnp.exp(decay_log) * step_size
    cumulative = jnp.cumsum(rate_step, axis=0).T
    length = sequence.shape[0]
    row_later = lax.broadcasted_iota(jnp.int32, (length, length), 0)
    earlier = lax.broadcasted_iota(jnp.int32, (length, length), 1)
    causal = row_later >= earlier
    log_decay = cumulative[:, None, :] - cumulative[:, :, None]
    decay_matrix = jnp.where(causal[None], jnp.exp(jnp.minimum(log_decay, 0.0)), 0.0)
    return (gram_matrix[None] * decay_matrix * step_size.T[:, None, :]).astype(jnp.bfloat16)


def on_device(
    tokens,
    teacher,
    inner_weight,
    output_weight,
    inner_first,
    inner_second,
    state_weight,
    step_weight,
    step_bias,
    decay_log,
    skip_gain,
):
    seq_rows, model_width = tokens.shape
    heads_here = step_weight.shape[1]
    groups_here = inner_weight.shape[1] // HEAD_DIM
    ratio = HEADS // GROUPS
    total_tokens = seq_rows * lax.axis_size(DP)
    whole = gathered(jnp.concatenate([inner_weight.astype(jnp.bfloat16), output_weight], axis=1))
    whole = whole.reshape(model_width, whole.shape[-1])
    inner_full, output_full = jnp.split(whole, [inner_weight.shape[1]], axis=1)
    weights_mix = mixing(tokens, state_weight, step_weight, step_bias, decay_log)
    projected = jnp.dot(tokens, inner_full, preferred_element_type=jnp.float32).astype(jnp.bfloat16)
    heads_in = jnp.repeat(projected.reshape(seq_rows, groups_here, HEAD_DIM), ratio, axis=1)
    mixed = jnp.einsum(
        "hts,shp->thp", weights_mix, heads_in, preferred_element_type=jnp.float32
    ) + skip_gain[None, :, None] * heads_in.astype(jnp.float32)
    inner = mixed.astype(jnp.bfloat16).reshape(seq_rows, heads_here * HEAD_DIM)
    inner_grad, sums = after_gather(
        inner, output_full, tokens, teacher, weights_mix,
        jnp.repeat(skip_gain, HEAD_DIM)[None, :], inner_weight.shape[0],
    )
    squares_total, error_total = sums[0, 0], sums[0, 1]
    entry_count = model_width * groups_here * HEAD_DIM * lax.axis_size("tensor")
    root_mean = jnp.sqrt(squares_total / entry_count)
    factor = jnp.minimum(1.0, 1.0 / (root_mean + norm_eps))
    distill_loss = error_total / (total_tokens * model_width)
    first_fix = 1.0 - beta_one**STEP
    second_fix = 1.0 - beta_two**STEP
    clipped = factor * inner_grad
    first_next = beta_one * inner_first + (1.0 - beta_one) * clipped
    second_next = beta_two * inner_second + (1.0 - beta_two) * clipped * clipped
    update = (
        first_next / first_fix / (jnp.sqrt(second_next / second_fix) + adam_eps)
        + weight_decay * inner_weight
    )
    return (distill_loss, update, first_next, second_next)


def solution(mesh):
    finer = Mesh(
        mesh.devices.reshape(8, 4, 2, 2, mesh.shape["tensor"]),
        ("dp_0", "dp_1", "dp_2", "dp_3", "tensor"),
    )
    return jax.shard_map(
        on_device,
        mesh=finer,
        in_specs=(
            P(DP, None),
            P(DP, None),
            P(DP, "tensor"),
            P(DP, "tensor"),
            P(DP, "tensor"),
            P(DP, "tensor"),
            P(),
            P(None, "tensor"),
            P("tensor"),
            P("tensor"),
            P("tensor"),
        ),
        out_specs=(P(), P(DP, "tensor"), P(DP, "tensor"), P(DP, "tensor")),
        check_vma=False,
    )
```

```python
import functools
import heapq

import jax
import jax.numpy as jnp
from jax import lax
from jax.experimental import pallas as pl
from jax.experimental.pallas import tpu as pltpu
from jax.sharding import Mesh
from jax.sharding import PartitionSpec as P

HEAD_DIM = 128
STEP = 20
DP = ("dp_0", "dp_1", "dp_2", "dp_3")


beta_one = 0.9
beta_two = 0.95
adam_eps = 1e-08
weight_decay = 0.1
norm_eps = 1e-06


TORUS = ("dp_0", "dp_1", "dp_2")
BY_COLUMN = ("dp_2", "dp_1", "dp_0")
BY_ROW = ("dp_2", "dp_0", "dp_1")
CHUNK = 256


def ways(sizes):
    def sign(rel, order):
        n, v = sizes[order[2]], rel[order[2]]
        if 2 * v == n:
            return 1 if (rel[order[0]] + rel[order[1]]) % 2 == 0 else -1
        return 1 if 2 * v < n else -1

    def onward(rel, order):
        last = order[2]
        n = sizes[last]
        if rel[last] == 0:
            moves = [1, -1] if n > 2 else [1]
        else:
            moves = [sign(rel, order)]
        out = []
        for move in moves:
            nxt = dict(rel)
            nxt[last] = (rel[last] + move) % n
            far = nxt[last] if move > 0 else n - nxt[last]
            was = rel[last] if move > 0 else (n - rel[last]) % n
            if nxt[last] and far == was + 1 and (n == 2 or sign(nxt, order) == move):
                out.append(nxt)
        return out

    def children(rel, order):
        out = onward(rel, order)
        if not any(rel.values()):
            for i in range(sizes[order[0]]):
                for j in range(sizes[order[1]]):
                    if i or j:
                        out.append({order[0]: i, order[1]: j, order[2]: 0})
            out.sort(key=lambda r: -sum(min(v, sizes[a] - v) for a, v in r.items()))
        return out

    return children


def relay_times(sizes, flows, latency=2.45, hop=0.45):
    children = ways(sizes)
    free, heap, count = {}, [], 0
    events = [[] for _ in flows]
    for n, (order, wire, start) in enumerate(flows):
        heapq.heappush(heap, (start, count, n, {a: 0 for a in TORUS}))
        count += 1
    while heap:
        now, _, n, rel = heapq.heappop(heap)
        order, wire, _ = flows[n]
        sends = children(rel, order)
        events[n].append((now, rel, sends))
        for nxt in sends:
            lands, hops = now, 0
            for a in TORUS:
                v = (nxt[a] - rel[a]) % sizes[a]
                if v:
                    go = 1 if 2 * v <= sizes[a] else -1
                    far = min(v, sizes[a] - v) * (2 if sizes[a] == 2 else 1)
                    begin = max(now, free.get((a, go), 0.0))
                    free[(a, go)] = begin + wire * far
                    lands = max(lands, begin + wire)
                    hops += far
            heapq.heappush(heap, (lands + latency + hop * (hops - 1), count, n, nxt))
            count += 1
    return events


def step_kernel(
    sizes, tokens, teacher, inner_weight, output_weight, state_weight, step_weight,
    step_bias, decay_log, skip, grad_out, sums_out,
    mine, in_all, w_all, mix, mix_t, inner,
    tok_t, tok_all, part, leaving, arrived, grad_acc, gp_all, g_part, g_all, row_a, row_b,
    in_send, in_recv, in_pair, w_send, w_recv, w_pair,
    student_send, student_recv, tok_send, tok_recv, gp_send, gp_recv,
    g_send, g_recv, a_send, a_recv, b_send, b_recv,
):
    axes = ("dp_0", "dp_1", "dp_2", "dp_3", "tensor")
    here = {a: lax.axis_index(a) for a in axes}
    nz, nx, ny = sizes["dp_0"], sizes["dp_1"], sizes["dp_2"]
    seq, features = tokens.shape
    cols = output_weight.shape[1]
    chunks = features // CHUNK
    heads = mix.shape[0]
    head_dim = cols // heads
    groups = inner_weight.shape[1] // head_dim
    per_group = heads // groups
    core = here["dp_3"]

    def ahead(a, v):
        return lax.rem(here[a] + (v % sizes[a]), sizes[a])

    def there(**by):
        return {a: ahead(a, v) for a, v in by.items() if v % sizes[a]}

    def remote(src, dst, send, recv, target):
        return pltpu.make_async_remote_copy(
            src, dst, send, recv, device_id=target, device_id_type=pl.DeviceIdType.MESH
        )

    plane = [
        dict(dp_1=i, dp_2=j, dp_3=k, tensor=t)
        for i in range(nx) for j in range(ny) for k in range(2) for t in range(2)
    ][1:]
    column = [dict(dp_0=i, dp_2=j) for i in range(nz) for j in range(ny)][1:]
    peers = plane + [by for by in column if by["dp_0"]]
    pair = there(dp_3=1)
    barrier = pltpu.get_barrier_semaphore()
    for by in peers:
        pl.semaphore_signal(
            barrier, inc=1, device_id=there(**by), device_id_type=pl.DeviceIdType.MESH
        )
    mine[...] = inner_weight[...].astype(jnp.bfloat16)
    in_all[here["dp_0"], here["dp_1"], here["dp_2"], core] = mine[...]
    w_all[here["dp_0"], here["dp_1"], here["dp_2"], core] = output_weight[...]

    in_wire, w_wire = 0.088, 0.352
    flows = (
        (BY_ROW, in_wire, 0.0), (BY_ROW, in_wire, 0.0),
        (BY_COLUMN, w_wire, 0.01), (BY_ROW, w_wire, 0.01),
    )
    events = relay_times(sizes, flows)
    steps = [
        sorted(
            [(t, 0, rel, sends) for t, rel, sends in events[c]]
            + [(t, 1, rel, sends) for t, rel, sends in events[2 + c]],
            key=lambda e: e[:2],
        )
        for c in range(2)
    ]

    def number(rel):
        return (rel["dp_0"] * nx + rel["dp_1"]) * ny + rel["dp_2"]

    def relay(c, begin, end):
        for time, kind, rel, sends in steps[c]:
            if not begin <= time < end:
                continue
            all_ref, own, send, recv = (
                (in_all, mine, in_send, in_recv), (w_all, output_weight, w_send, w_recv)
            )[kind]
            at = tuple(ahead(a, -rel[a]) for a in TORUS)
            slot = all_ref.at[at[0], at[1], at[2], c]
            first = not any(rel.values())
            block = own if first else slot
            if not first:
                remote(slot, slot, send, recv.at[number(rel)], pair).wait_recv()
            for nxt in sends:
                target = there(**{a: nxt[a] - rel[a] for a in TORUS})
                remote(block, slot, send, recv.at[number(nxt)], target).start()
            beside = in_pair if kind == 0 else w_pair.at[rel["dp_0"]]
            remote(block, slot, send, beside, pair).start()

    def relay_until(begin, end):
        for c in range(2):
            @pl.when(core == c)
            def _():
                relay(c, begin, end)

    def turn_tokens():
        per = tok_t.shape[4]
        rows_x = ny * 2 * per
        for k in range(features // 128):
            turned = tokens[:, k * 128 : (k + 1) * 128].T
            z, x = divmod(k * 128 // rows_x, nx)
            tok_t[z, x : x + 128 // rows_x] = turned.reshape(128 // rows_x, ny, 2, per, seq)

    def mix_heads():
        projected = jnp.dot(tokens[...], state_weight[...], preferred_element_type=jnp.float32)
        width = projected.shape[1] // 2
        b_coef, c_coef = projected[:, :width], projected[:, width:]
        gram = lax.dot_general(
            c_coef, b_coef, (((1,), (1,)), ((), ())),
            precision=lax.Precision.HIGHEST, preferred_element_type=jnp.float32,
        )
        raw = (
            jnp.dot(tokens[...], step_weight[...], preferred_element_type=jnp.float32)
            + step_bias[...]
        )
        step_size = jnp.maximum(raw, 0.0) + jnp.log1p(jnp.exp(-jnp.abs(raw)))
        rate = jnp.exp(decay_log[...]) * step_size
        later = lax.broadcasted_iota(jnp.int32, (seq, seq), 0)
        earlier = lax.broadcasted_iota(jnp.int32, (seq, seq), 1)
        causal = later >= earlier
        cumulative = jnp.dot(
            causal.astype(jnp.float32), rate,
            precision=lax.Precision.HIGHEST, preferred_element_type=jnp.float32,
        )
        blank = jnp.zeros((seq, seq - heads), jnp.float32)
        cum_t = jnp.concatenate([cumulative, blank], axis=1).T
        step_t = jnp.concatenate([step_size, blank], axis=1).T
        for h in range(heads):
            log_decay = cum_t[h : h + 1, :] - cumulative[:, h : h + 1]
            decay = jnp.where(causal, jnp.exp(jnp.minimum(log_decay, 0.0)), 0.0)
            mix[h] = (gram * decay * step_t[h : h + 1, :]).astype(jnp.bfloat16)

    def turn_mix():
        for g in range(groups):
            for h in range(per_group):
                mix_t[g, :, h * seq : (h + 1) * seq] = mix[g * per_group + h].T

    def project():
        width = inner_weight.shape[1]
        projected = jnp.dot(
            tokens[...], in_all[...].reshape(features, width),
            preferred_element_type=jnp.float32,
        ).astype(jnp.bfloat16)
        for g in range(groups):
            source = projected[:, g * head_dim : (g + 1) * head_dim]
            stack = mix[g * per_group : (g + 1) * per_group].reshape(per_group * seq, seq)
            mixed = jnp.dot(stack, source, preferred_element_type=jnp.float32)
            wide = source.astype(jnp.float32)
            for h in range(per_group):
                n = g * per_group + h
                inner[:, n * head_dim : (n + 1) * head_dim] = (
                    mixed[h * seq : (h + 1) * seq] + skip[:, n : n + 1] * wide
                ).astype(jnp.bfloat16)

    other_half = there(tensor=1)
    order = sorted(range(nz), key=lambda v: (min(v, nz - v), v))

    def student_copy(i):
        return remote(
            leaving.at[i], arrived.at[i], student_send, student_recv.at[i], other_half
        )

    def w_rows(i):
        return w_all[ahead("dp_0", -order[i])].reshape(CHUNK, cols)

    def teacher_cols(i):
        return teacher[:, pl.ds(pl.multiple_of(ahead("dp_0", -order[i]) * CHUNK, CHUNK), CHUNK)]

    def student(i):
        beside = w_all.at[0, :, :, 0]
        remote(beside, beside, w_send, w_pair.at[order[i]], pair).wait_recv()
        piece = lax.dot_general(
            inner[...], w_rows(i), (((1,), (1,)), ((), ())), preferred_element_type=jnp.float32
        )
        part[i] = piece
        leaving[i] = piece.astype(jnp.bfloat16)
        if i:
            student_copy(i - 1).start()

    pl.semaphore_wait(barrier, len(peers))
    late = max(t for t, *_ in steps[0] + steps[1]) + 1
    inner_done = max(t for c in range(2) for t, kind, *_ in steps[c] if kind == 0) + 1e-6
    relay_until(0, 2.0)
    turn_tokens()
    relay_until(2.0, 6.0)
    mix_heads()
    relay_until(6.0, 9.0)
    turn_mix()
    relay_until(9.0, max(inner_done, 9.0))
    beside = in_all.at[:, :, :, 0]
    remote(beside, beside, in_send, in_pair, pair).wait_recv()
    project()
    reached = max(inner_done, 9.0)
    for i in range(chunks):
        needed = max(
            t for c in range(2) for t, kind, rel, _ in steps[c]
            if kind == 1 and rel["dp_0"] == order[i]
        ) + 1e-6
        if needed > reached:
            relay_until(reached, needed)
            reached = needed
        student(i)
    relay_until(reached, late)
    student_copy(chunks - 1).start()

    tok_sends = []
    for i in range(nx):
        for k in range(2):
            slot = i * 2 + k
            to_x = lax.rem(here["dp_1"] + i, nx)
            to_c = lax.rem(here["dp_3"] + k, 2)
            if slot:
                tok_sends.append((slot, to_x, to_c, there(dp_1=i, dp_3=k)))
    for slot, to_x, to_c, target in tok_sends:
        remote(
            tok_t.at[:, to_x, :, to_c], tok_all.at[slot], tok_send, tok_recv, target
        ).start()
    tok_all[0] = tok_t[:, here["dp_1"], :, here["dp_3"]]

    squares = jnp.zeros((8, CHUNK), jnp.float32)
    for i in range(chunks):
        student_copy(i).wait_recv()
        error = (
            part[i] + arrived[i].astype(jnp.float32)
            - teacher_cols(i).astype(jnp.float32)
        )
        squares = squares + jnp.sum((error * error).reshape(seq // 8, 8, CHUNK), axis=0)
        product = jnp.dot(
            error.astype(jnp.bfloat16), w_rows(i), preferred_element_type=jnp.float32,
        )
        if i == 0:
            grad_acc[...] = product
        else:
            grad_acc[...] += product
    for g in range(groups):
        heads = []
        direct = None
        for h in range(per_group):
            at = slice((g * per_group + h) * head_dim, (g * per_group + h + 1) * head_dim)
            one = grad_acc[:, at].astype(jnp.bfloat16)
            heads.append(one)
            n = g * per_group + h
            term = skip[:, n : n + 1] * one.astype(jnp.float32)
            direct = term if direct is None else direct + term
        back = jnp.dot(
            mix_t[g], jnp.concatenate(heads, axis=0), preferred_element_type=jnp.float32
        )
        gp_all[0, :, g * head_dim : (g + 1) * head_dim] = (back + direct).astype(jnp.bfloat16)

    for i in (2, 1, 3) if nx == 4 else range(1, nx):
        remote(
            gp_all.at[0], gp_all.at[2 * i], gp_send, gp_recv.at[2 * i], there(dp_1=i)
        ).start()
    remote(gp_all.at[0], gp_all.at[1], gp_send, gp_recv.at[1], pair).start()
    members = 2 * nx
    remote(
        tok_all.at[pl.ds(1, members - 1)], tok_all.at[pl.ds(1, members - 1)],
        tok_send, tok_recv, pair,
    ).wait()

    def product_of(slot):
        left = tok_all[slot].reshape(-1, seq)
        return jnp.dot(left, gp_all[slot], preferred_element_type=jnp.float32)

    remote(gp_all.at[1], gp_all.at[1], gp_send, gp_recv.at[1], pair).wait_recv()
    total = product_of(0) + product_of(1)
    near = (1, 3, 2) if nx == 4 else range(1, nx)
    for i in near:
        remote(gp_all.at[0], gp_all.at[2 * i], gp_send, gp_recv.at[2 * i], pair).wait_recv()
        remote(
            gp_all.at[2 * i], gp_all.at[2 * i + 1], gp_send, gp_recv.at[2 * i + 1], pair
        ).start()
        total = total + product_of(2 * i)
    for i in near:
        remote(
            gp_all.at[0], gp_all.at[2 * i + 1], gp_send, gp_recv.at[2 * i + 1], pair
        ).wait_recv()
        total = total + product_of(2 * i + 1)
    g_part[...] = total.reshape(g_part.shape)

    for by in sorted(column, key=lambda b: -min(b["dp_0"], nz - b["dp_0"]) - b["dp_2"]):
        slot = by["dp_0"] * ny + by["dp_2"]
        to_z = lax.rem(here["dp_0"] + by["dp_0"], nz)
        to_y = lax.rem(here["dp_2"] + by["dp_2"], ny)
        remote(g_part.at[to_z, to_y], g_all.at[slot], g_send, g_recv, there(**by)).start()
    g_all[0] = g_part[here["dp_0"], here["dp_2"]]
    err = jnp.sum(squares) * 0.5
    rest = g_all.at[pl.ds(1, nz * ny - 1)]
    remote(rest, rest, g_send, g_recv, pair).wait()
    grad = jnp.sum(g_all[...], axis=0)
    grad_out[...] = grad
    lane = lax.broadcasted_iota(jnp.int32, (1, 128), 1)
    row = jnp.where(lane == 0, jnp.sum(grad * grad), jnp.where(lane == 1, err, 0.0))
    row_a[0] = row
    for n, by in enumerate(plane):
        remote(row_a.at[0], row_a.at[n + 1], a_send, a_recv, there(**by)).start()
    rest = row_a.at[pl.ds(1, len(plane))]
    remote(rest, rest, a_send, a_recv, pair).wait()
    row_b[0] = jnp.sum(row_a[...], axis=0)
    for i in range(1, nz):
        remote(row_b.at[0], row_b.at[i], b_send, b_recv, there(dp_0=i)).start()
    rest = row_b.at[pl.ds(1, nz - 1)]
    remote(rest, rest, b_send, b_recv, pair).wait()
    sums_out[...] = jnp.sum(row_b[...], axis=0)

    rest = gp_all.at[pl.ds(1, members - 1)]
    remote(rest, rest, gp_send, gp_recv.at[1], pair).wait_send()
    remote(leaving, leaving, student_send, student_recv.at[0], pair).wait_send()
    pieces = nz * nx * ny
    for block, ref, send in (((0,), in_all, in_send), ((0,), w_all, w_send)):
        half = ref.at[:, :, :, 0]
        remote(half, half, send, in_pair, pair).wait_send()
        rest = ref.at[pl.ds(0, nz - 1), :, :, 0]
        remote(rest, rest, send, in_pair, pair).wait_send()
        rest = ref.at[0, pl.ds(0, nx - 1), :, 0]
        remote(rest, rest, send, in_pair, pair).wait_send()
        rest = ref.at[0, 0, pl.ds(0, ny - 1), 0]
        remote(rest, rest, send, in_pair, pair).wait_send()


def whole_step(
    tokens, teacher, inner_weight, output_weight, state_weight, step_weight,
    step_bias, decay_log, skip_gain,
):
    sizes = {a: lax.axis_size(a) for a in ("dp_0", "dp_1", "dp_2", "dp_3", "tensor")}
    nz, nx, ny = sizes["dp_0"], sizes["dp_1"], sizes["dp_2"]
    seq, features = tokens.shape
    own_rows, cols = output_weight.shape
    gcols = inner_weight.shape[1]
    heads = step_weight.shape[1]
    chunks = features // CHUNK
    groups = gcols // HEAD_DIM
    f32, half = jnp.float32, jnp.bfloat16
    vmem = pl.BlockSpec(memory_space=pltpu.VMEM)
    dma = pltpu.SemaphoreType.DMA
    return pl.pallas_call(
        functools.partial(step_kernel, sizes),
        name="whole_step",
        out_shape=(
            jax.ShapeDtypeStruct((own_rows, gcols), f32),
            jax.ShapeDtypeStruct((1, 128), f32),
        ),
        in_specs=[vmem] * 9,
        out_specs=(vmem, vmem),
        scratch_shapes=[
            pltpu.VMEM((own_rows, gcols), half),
            pltpu.VMEM((nz, nx, ny, 2, own_rows, gcols), half),
            pltpu.VMEM((nz, nx, ny, 2, own_rows, cols), half),
            pltpu.VMEM((heads, seq, seq), half),
            pltpu.VMEM((groups, seq, heads // groups * seq), half),
            pltpu.VMEM((seq, cols), half),
            pltpu.VMEM((nz, nx, ny, 2, own_rows, seq), half),
            pltpu.VMEM((2 * nx, nz, ny, own_rows, seq), half),
            pltpu.VMEM((chunks, seq, CHUNK), f32),
            pltpu.VMEM((chunks, seq, CHUNK), half),
            pltpu.VMEM((chunks, seq, CHUNK), half),
            pltpu.VMEM((seq, cols), f32),
            pltpu.VMEM((2 * nx, seq, gcols), half),
            pltpu.VMEM((nz, ny, own_rows, gcols), f32),
            pltpu.VMEM((nz * ny, own_rows, gcols), f32),
            pltpu.VMEM((nx * ny * 4, 1, 128), f32),
            pltpu.VMEM((nz, 1, 128), f32),
            dma, dma((nz * nx * ny,)), dma, dma, dma((nz * nx * ny,)), dma((nz,)),
            dma, dma((chunks,)), dma, dma, dma, dma((2 * nx,)),
            dma, dma, dma, dma, dma, dma,
        ],
        compiler_params=pltpu.CompilerParams(
            collective_id=0, has_side_effects=True, vmem_limit_bytes=40 * 1024 * 1024
        ),
    )(
        tokens, teacher, inner_weight, output_weight, state_weight, step_weight,
        step_bias[None, :], decay_log[None, :], skip_gain[None, :],
    )


def on_device(
    tokens,
    teacher,
    inner_weight,
    output_weight,
    inner_first,
    inner_second,
    state_weight,
    step_weight,
    step_bias,
    decay_log,
    skip_gain,
):
    seq_rows, model_width = tokens.shape
    groups_here = inner_weight.shape[1] // HEAD_DIM
    total_tokens = seq_rows * lax.axis_size(DP)
    inner_grad, sums = whole_step(
        tokens, teacher, inner_weight, output_weight, state_weight, step_weight,
        step_bias, decay_log, skip_gain,
    )
    squares_total, error_total = sums[0, 0], sums[0, 1]
    entry_count = model_width * groups_here * HEAD_DIM * lax.axis_size("tensor")
    root_mean = jnp.sqrt(squares_total / entry_count)
    factor = jnp.minimum(1.0, 1.0 / (root_mean + norm_eps))
    distill_loss = error_total / (total_tokens * model_width)
    first_fix = 1.0 - beta_one**STEP
    second_fix = 1.0 - beta_two**STEP
    clipped = factor * inner_grad
    first_next = beta_one * inner_first + (1.0 - beta_one) * clipped
    second_next = beta_two * inner_second + (1.0 - beta_two) * clipped * clipped
    update = (
        first_next / first_fix / (jnp.sqrt(second_next / second_fix) + adam_eps)
        + weight_decay * inner_weight
    )
    return (distill_loss, update, first_next, second_next)


def solution(mesh):
    finer = Mesh(
        mesh.devices.reshape(8, 4, 2, 2, mesh.shape["tensor"]),
        ("dp_0", "dp_1", "dp_2", "dp_3", "tensor"),
    )
    return jax.shard_map(
        on_device,
        mesh=finer,
        in_specs=(
            P(DP, None),
            P(DP, None),
            P(DP, "tensor"),
            P(DP, "tensor"),
            P(DP, "tensor"),
            P(DP, "tensor"),
            P(),
            P(None, "tensor"),
            P("tensor"),
            P("tensor"),
            P("tensor"),
        ),
        out_specs=(P(), P(DP, "tensor"), P(DP, "tensor"), P(DP, "tensor")),
        check_vma=False,
    )
```

```python
import functools
import heapq

import jax
import jax.numpy as jnp
from jax import lax
from jax.experimental import pallas as pl
from jax.experimental.pallas import tpu as pltpu
from jax.sharding import Mesh
from jax.sharding import PartitionSpec as P

HEAD_DIM = 128
STEP = 20
DP = ("dp_0", "dp_1", "dp_2", "dp_3")


beta_one = 0.9
beta_two = 0.95
adam_eps = 1e-08
weight_decay = 0.1
norm_eps = 1e-06


TORUS = ("dp_0", "dp_1", "dp_2")
BY_COLUMN = (("dp_2", "dp_1", "dp_0"), 2)
BY_ROW = (("dp_0", "dp_2", "dp_1"), 1)
CHUNK = 256


def ways(sizes):
    def sign(rel, order):
        n, v = sizes[order[2]], rel[order[2]]
        if 2 * v == n:
            return 1 if (rel[order[0]] + rel[order[1]]) % 2 == 0 else -1
        return 1 if 2 * v < n else -1

    def onward(rel, order):
        last = order[2]
        n = sizes[last]
        if rel[last] == 0:
            moves = [1, -1] if n > 2 else [1]
        else:
            moves = [sign(rel, order)]
        out = []
        for move in moves:
            nxt = dict(rel)
            nxt[last] = (rel[last] + move) % n
            far = nxt[last] if move > 0 else n - nxt[last]
            was = rel[last] if move > 0 else (n - rel[last]) % n
            if nxt[last] and far == was + 1 and (n == 2 or sign(nxt, order) == move):
                out.append(nxt)
        return out

    def children(rel, tree):
        order, straight = tree
        out = onward(rel, order)
        zero = {a: 0 for a in TORUS}
        if not any(rel.values()):
            for i in range(sizes[order[0]]):
                for j in range(sizes[order[1]] if straight == 2 else 1):
                    if i or j:
                        out.append({**zero, order[0]: i, order[1]: j})
        if straight == 1 and rel[order[1]] == 0 and rel[order[2]] == 0:
            out += [{**rel, order[1]: j} for j in range(1, sizes[order[1]])]
        out.sort(key=lambda r: -sum(min(v, sizes[a] - v) for a, v in r.items()))
        return out

    return children


def relay_times(sizes, flows, latency=2.45, hop=0.45):
    children = ways(sizes)
    free, heap, count = {}, [], 0
    events = [[] for _ in flows]
    for n, (order, wire, start) in enumerate(flows):
        heapq.heappush(heap, (start, count, n, {a: 0 for a in TORUS}))
        count += 1
    while heap:
        now, _, n, rel = heapq.heappop(heap)
        order, wire, _ = flows[n]
        sends = children(rel, order)
        events[n].append((now, rel, sends))
        for nxt in sends:
            lands, hops = now, 0
            for a in TORUS:
                v = (nxt[a] - rel[a]) % sizes[a]
                if v:
                    go = 1 if 2 * v <= sizes[a] else -1
                    far = min(v, sizes[a] - v) * (2 if sizes[a] == 2 else 1)
                    begin = max(now, free.get((a, go), 0.0))
                    free[(a, go)] = begin + wire * far
                    lands = max(lands, begin + wire)
                    hops += far
            heapq.heappush(heap, (lands + latency + hop * (hops - 1), count, n, nxt))
            count += 1
    return events


def step_kernel(
    sizes,
    tokens_hbm, teacher_hbm, inner_weight_hbm, output_weight_hbm, state_weight_hbm,
    step_weight_hbm, step_bias_hbm, decay_log_hbm, skip_hbm,
    loss_out, clipped_out,
    tokens, teacher, inner_weight, output_weight, state_weight,
    step_weight, step_bias, decay_log, skip, load_sem,
    mine, in_all, w_all, mix, mix_t, inner,
    tok_t, tok_all, part, leaving, arrived, grad_acc, gp_all, g_part, g_all, row_a, row_b,
    in_send, in_recv, in_pair, w_send, w_recv, w_pair,
    student_send, student_recv, tok_send, tok_recv, gp_send, gp_recv,
    g_send, g_recv, a_send, a_recv, b_send, b_recv,
):
    axes = ("dp_0", "dp_1", "dp_2", "dp_3", "tensor")
    here = {a: lax.axis_index(a) for a in axes}
    nz, nx, ny = sizes["dp_0"], sizes["dp_1"], sizes["dp_2"]
    seq, features = tokens.shape
    cols = output_weight.shape[1]
    chunks = features // CHUNK
    heads = mix.shape[0]
    head_dim = cols // heads
    groups = inner_weight.shape[1] // head_dim
    per_group = heads // groups
    core = here["dp_3"]

    def ahead(a, v):
        return lax.rem(here[a] + (v % sizes[a]), sizes[a])

    def there(**by):
        return {a: ahead(a, v) for a, v in by.items() if v % sizes[a]}

    def remote(src, dst, send, recv, target):
        return pltpu.make_async_remote_copy(
            src, dst, send, recv, device_id=target, device_id_type=pl.DeviceIdType.MESH
        )

    plane = [
        dict(dp_1=i, dp_2=j, dp_3=k, tensor=t)
        for i in range(nx) for j in range(ny) for k in range(2) for t in range(2)
    ][1:]
    column = [dict(dp_0=i, dp_2=j) for i in range(nz) for j in range(ny)][1:]
    peers = plane + [dict(dp_0=i) for i in range(1, nz)]
    pair = there(dp_3=1)
    loads = [
        pltpu.make_async_copy(source, target, load_sem.at[n])
        for n, (source, target) in enumerate((
            (inner_weight_hbm, inner_weight), (output_weight_hbm, output_weight),
            (tokens_hbm, tokens), (state_weight_hbm, state_weight),
            (step_weight_hbm, step_weight), (step_bias_hbm, step_bias),
            (decay_log_hbm, decay_log), (skip_hbm, skip), (teacher_hbm, teacher),
        ))
    ]
    for load in loads:
        load.start()
    barrier = pltpu.get_barrier_semaphore()
    for by in peers:
        pl.semaphore_signal(
            barrier, inc=1, device_id=there(**by), device_id_type=pl.DeviceIdType.MESH
        )
    for load in loads[:2]:
        load.wait()
    mine[...] = inner_weight[...].astype(jnp.bfloat16)
    in_all[here["dp_0"], here["dp_1"], here["dp_2"], core] = mine[...]
    w_all[here["dp_0"], here["dp_1"], here["dp_2"], core] = output_weight[...]

    in_wire, w_wire = 0.088, 0.352
    flows = (
        (BY_ROW, in_wire, 0.0), (BY_ROW, in_wire, 0.0),
        (BY_COLUMN, w_wire, 0.01), (BY_COLUMN, w_wire, 0.01),
    )
    events = relay_times(sizes, flows)
    steps = [
        sorted(
            [(t, 0, rel, sends) for t, rel, sends in events[c]]
            + [(t, 1, rel, sends) for t, rel, sends in events[2 + c]],
            key=lambda e: e[:2],
        )
        for c in range(2)
    ]

    def number(rel):
        return (rel["dp_0"] * nx + rel["dp_1"]) * ny + rel["dp_2"]

    def relay(c, begin, end):
        for time, kind, rel, sends in steps[c]:
            if not begin <= time < end:
                continue
            all_ref, own, send, recv = (
                (in_all, mine, in_send, in_recv), (w_all, output_weight, w_send, w_recv)
            )[kind]
            at = tuple(ahead(a, -rel[a]) for a in TORUS)
            slot = all_ref.at[at[0], at[1], at[2], c]
            first = not any(rel.values())
            block = own if first else slot
            if not first:
                remote(slot, slot, send, recv.at[number(rel)], pair).wait_recv()
            for nxt in sends:
                target = there(**{a: nxt[a] - rel[a] for a in TORUS})
                remote(block, slot, send, recv.at[number(nxt)], target).start()
            beside = in_pair if kind == 0 else w_pair.at[rel["dp_0"]]
            remote(block, slot, send, beside, pair).start()

    def relay_until(begin, end):
        for c in range(2):
            @pl.when(core == c)
            def _():
                relay(c, begin, end)

    def turn_tokens():
        per = tok_t.shape[4]
        rows_x = ny * 2 * per
        for k in range(features // 128):
            turned = tokens[:, k * 128 : (k + 1) * 128].T
            z, x = divmod(k * 128 // rows_x, nx)
            tok_t[z, x : x + 128 // rows_x] = turned.reshape(128 // rows_x, ny, 2, per, seq)

    def mix_heads():
        projected = lax.dot_general(
            tokens[...], state_weight[...], (((1,), (1,)), ((), ())),
            preferred_element_type=jnp.float32,
        )
        width = projected.shape[1] // 2
        b_coef, c_coef = projected[:, :width], projected[:, width:]
        gram = lax.dot_general(
            c_coef, b_coef, (((1,), (1,)), ((), ())),
            precision=lax.Precision.HIGHEST, preferred_element_type=jnp.float32,
        )
        raw = (
            lax.dot_general(
                tokens[...], step_weight[...], (((1,), (1,)), ((), ())),
                preferred_element_type=jnp.float32,
            )
            + step_bias[...]
        )
        step_size = jnp.maximum(raw, 0.0) + jnp.log1p(jnp.exp(-jnp.abs(raw)))
        rate = jnp.exp(decay_log[...]) * step_size
        later = lax.broadcasted_iota(jnp.int32, (seq, seq), 0)
        earlier = lax.broadcasted_iota(jnp.int32, (seq, seq), 1)
        causal = later >= earlier
        cumulative = jnp.dot(
            causal.astype(jnp.float32), rate,
            precision=lax.Precision.HIGHEST, preferred_element_type=jnp.float32,
        )
        blank = jnp.zeros((seq, seq - heads), jnp.float32)
        cum_t = jnp.concatenate([cumulative, blank], axis=1).T
        step_t = jnp.concatenate([step_size, blank], axis=1).T
        for h in range(heads):
            log_decay = cum_t[h : h + 1, :] - cumulative[:, h : h + 1]
            decay = jnp.where(causal, jnp.exp(jnp.minimum(log_decay, 0.0)), 0.0)
            mix[h] = (gram * decay * step_t[h : h + 1, :]).astype(jnp.bfloat16)

    def turn_mix():
        for g in range(groups):
            for h in range(per_group):
                mix_t[g, :, h * seq : (h + 1) * seq] = mix[g * per_group + h].T

    def project():
        width = inner_weight.shape[1]
        projected = jnp.dot(
            tokens[...], in_all[...].reshape(features, width),
            preferred_element_type=jnp.float32,
        ).astype(jnp.bfloat16)
        for g in range(groups):
            source = projected[:, g * head_dim : (g + 1) * head_dim]
            stack = mix[g * per_group : (g + 1) * per_group].reshape(per_group * seq, seq)
            mixed = jnp.dot(stack, source, preferred_element_type=jnp.float32)
            wide = source.astype(jnp.float32)
            for h in range(per_group):
                n = g * per_group + h
                inner[:, n * head_dim : (n + 1) * head_dim] = (
                    mixed[h * seq : (h + 1) * seq] + skip[:, n : n + 1] * wide
                ).astype(jnp.bfloat16)

    other_half = there(tensor=1)
    order = sorted(range(nz), key=lambda v: (min(v, nz - v), v))

    def student_copy(i):
        return remote(
            leaving.at[i], arrived.at[i], student_send, student_recv.at[i], other_half
        )

    def w_rows(i):
        return w_all[ahead("dp_0", -order[i])].reshape(CHUNK, cols)

    def teacher_cols(i):
        return teacher[:, pl.ds(pl.multiple_of(ahead("dp_0", -order[i]) * CHUNK, CHUNK), CHUNK)]

    def student(i):
        beside = w_all.at[0, :, :, 0]
        remote(beside, beside, w_send, w_pair.at[order[i]], pair).wait_recv()
        piece = lax.dot_general(
            inner[...], w_rows(i), (((1,), (1,)), ((), ())), preferred_element_type=jnp.float32
        )
        part[i] = piece
        leaving[i] = piece.astype(jnp.bfloat16)
        if i:
            student_copy(i - 1).start()

    pl.semaphore_wait(barrier, len(peers))
    late = max(t for t, *_ in steps[0] + steps[1]) + 1
    inner_done = max(t for c in range(2) for t, kind, *_ in steps[c] if kind == 0) + 1e-6
    relay_until(0, 2.0)
    for load in loads[2:]:
        load.wait()
    turn_tokens()
    relay_until(2.0, 6.0)
    mix_heads()
    relay_until(6.0, 9.0)
    turn_mix()
    relay_until(9.0, max(inner_done, 9.0))
    beside = in_all.at[:, :, :, 0]
    remote(beside, beside, in_send, in_pair, pair).wait_recv()
    project()
    tok_sends = []
    for i in range(nx):
        for k in range(2):
            slot = i * 2 + k
            to_x = lax.rem(here["dp_1"] + i, nx)
            to_c = lax.rem(here["dp_3"] + k, 2)
            if slot:
                tok_sends.append((slot, to_x, to_c, there(dp_1=i, dp_3=k)))
    for slot, to_x, to_c, target in tok_sends:
        remote(
            tok_t.at[:, to_x, :, to_c], tok_all.at[slot], tok_send, tok_recv, target
        ).start()
    tok_all[0] = tok_t[:, here["dp_1"], :, here["dp_3"]]

    reached = max(inner_done, 9.0)
    for i in range(chunks):
        needed = max(
            t for c in range(2) for t, kind, rel, _ in steps[c]
            if kind == 1 and rel["dp_0"] == order[i]
        ) + 1e-6
        if needed > reached:
            relay_until(reached, needed)
            reached = needed
        student(i)
    relay_until(reached, late)
    student_copy(chunks - 1).start()

    squares = jnp.zeros((8, CHUNK), jnp.float32)
    for i in range(chunks):
        student_copy(i).wait_recv()
        error = (
            part[i] + arrived[i].astype(jnp.float32)
            - teacher_cols(i).astype(jnp.float32)
        )
        squares = squares + jnp.sum((error * error).reshape(seq // 8, 8, CHUNK), axis=0)
        product = jnp.dot(
            error.astype(jnp.bfloat16), w_rows(i), preferred_element_type=jnp.float32,
        )
        if i == 0:
            grad_acc[...] = product
        else:
            grad_acc[...] += product
    near = (1, 3, 2) if nx == 4 else range(1, nx)
    members = 2 * nx

    def gp_copy(g, source, slot, target):
        return remote(
            gp_all.at[g, source], gp_all.at[g, slot], gp_send, gp_recv.at[g, slot], target
        )

    for g in range(groups):
        heads_here = []
        direct = None
        for h in range(per_group):
            n = g * per_group + h
            one = grad_acc[:, n * head_dim : (n + 1) * head_dim].astype(jnp.bfloat16)
            heads_here.append(one)
            term = skip[:, n : n + 1] * one.astype(jnp.float32)
            direct = term if direct is None else direct + term
        back = jnp.dot(
            mix_t[g], jnp.concatenate(heads_here, axis=0), preferred_element_type=jnp.float32
        )
        gp_all[g, 0] = (back + direct).astype(jnp.bfloat16)
        for i in reversed(near):
            gp_copy(g, 0, 2 * i, there(dp_1=i)).start()
        gp_copy(g, 0, 1, pair).start()
    remote(
        tok_all.at[pl.ds(1, members - 1)], tok_all.at[pl.ds(1, members - 1)],
        tok_send, tok_recv, pair,
    ).wait()

    def product_of(g, slot):
        left = tok_all[slot].reshape(-1, seq)
        return jnp.dot(left, gp_all[g, slot], preferred_element_type=jnp.float32)

    outward = sorted(column, key=lambda b: -min(b["dp_0"], nz - b["dp_0"]) - b["dp_2"])
    for g in range(groups):
        gp_copy(g, 1, 1, pair).wait_recv()
        total = product_of(g, 0) + product_of(g, 1)
        for i in near:
            gp_copy(g, 0, 2 * i, pair).wait_recv()
            gp_copy(g, 2 * i, 2 * i + 1, pair).start()
            total = total + product_of(g, 2 * i)
        for i in near:
            gp_copy(g, 0, 2 * i + 1, pair).wait_recv()
            total = total + product_of(g, 2 * i + 1)
        g_part[g] = total.reshape(g_part.shape[1:])
        for by in outward:
            slot = by["dp_0"] * ny + by["dp_2"]
            to_z, to_y = ahead("dp_0", by["dp_0"]), ahead("dp_2", by["dp_2"])
            remote(
                g_part.at[g, to_z, to_y], g_all.at[g, slot], g_send, g_recv.at[g], there(**by)
            ).start()
        g_all[g, 0] = g_part[g, here["dp_0"], here["dp_2"]]
    err = jnp.sum(squares) * 0.5
    halves = []
    for g in range(groups):
        rest = g_all.at[g, pl.ds(1, nz * ny - 1)]
        remote(rest, rest, g_send, g_recv.at[g], pair).wait_recv()
        halves.append(jnp.sum(g_all[g], axis=0))
    grad = jnp.concatenate(halves, axis=1)
    lane = lax.broadcasted_iota(jnp.int32, (1, 128), 1)
    row = jnp.where(lane == 0, jnp.sum(grad * grad), jnp.where(lane == 1, err, 0.0))
    row_a[0] = row
    for n, by in enumerate(plane):
        remote(row_a.at[0], row_a.at[n + 1], a_send, a_recv, there(**by)).start()
    rest = row_a.at[pl.ds(1, len(plane))]
    remote(rest, rest, a_send, a_recv, pair).wait()
    row_b[0] = jnp.sum(row_a[...], axis=0)
    for i in range(1, nz):
        remote(row_b.at[0], row_b.at[i], b_send, b_recv, there(dp_0=i)).start()
    rest = row_b.at[pl.ds(1, nz - 1)]
    remote(rest, rest, b_send, b_recv, pair).wait()
    sums = jnp.sum(row_b[...], axis=0)
    root_mean = jnp.sqrt(sums[:, 0:1] / (features * inner_weight.shape[1] * 2))
    factor = jnp.minimum(1.0, 1.0 / (root_mean + norm_eps))
    loss_out[...] = jnp.broadcast_to(sums[:, 1:2] / (nz * nx * ny * 2 * seq * features), (1, 128))
    clipped_out[...] = factor * grad
    for g in range(groups):
        rest = gp_all.at[g, pl.ds(1, members - 1)]
        remote(rest, rest, gp_send, gp_recv.at[g, 1], pair).wait_send()
        rest = g_all.at[g, pl.ds(1, nz * ny - 1)]
        remote(rest, rest, g_send, g_recv.at[g], pair).wait_send()
    remote(leaving, leaving, student_send, student_recv.at[0], pair).wait_send()
    pieces = nz * nx * ny
    for block, ref, send in (((0,), in_all, in_send), ((0,), w_all, w_send)):
        half = ref.at[:, :, :, 0]
        remote(half, half, send, in_pair, pair).wait_send()
        rest = ref.at[pl.ds(0, nz - 1), :, :, 0]
        remote(rest, rest, send, in_pair, pair).wait_send()
        rest = ref.at[0, pl.ds(0, nx - 1), :, 0]
        remote(rest, rest, send, in_pair, pair).wait_send()
        rest = ref.at[0, 0, pl.ds(0, ny - 1), 0]
        remote(rest, rest, send, in_pair, pair).wait_send()


def whole_step(
    tokens, teacher, inner_weight, output_weight, state_weight, step_weight,
    step_bias, decay_log, skip_gain,
):
    sizes = {a: lax.axis_size(a) for a in ("dp_0", "dp_1", "dp_2", "dp_3", "tensor")}
    nz, nx, ny = sizes["dp_0"], sizes["dp_1"], sizes["dp_2"]
    seq, features = tokens.shape
    own_rows, cols = output_weight.shape
    gcols = inner_weight.shape[1]
    heads = step_weight.shape[1]
    chunks = features // CHUNK
    groups = gcols // HEAD_DIM
    f32, half = jnp.float32, jnp.bfloat16
    vmem = pl.BlockSpec(memory_space=pltpu.VMEM)
    dma = pltpu.SemaphoreType.DMA
    return pl.pallas_call(
        functools.partial(step_kernel, sizes),
        name="whole_step",
        out_shape=(
            jax.ShapeDtypeStruct((1, 128), f32),
            jax.ShapeDtypeStruct((own_rows, gcols), f32),
        ),
        in_specs=[pl.BlockSpec(memory_space=pl.ANY)] * 9,
        out_specs=(vmem,) * 2,
        scratch_shapes=[
            pltpu.VMEM((seq, features), half),
            pltpu.VMEM((seq, features), half),
            pltpu.VMEM((own_rows, gcols), f32),
            pltpu.VMEM((own_rows, cols), half),
            pltpu.VMEM((state_weight.shape[1], features), half),
            pltpu.VMEM((heads, features), half),
            pltpu.VMEM((1, heads), f32),
            pltpu.VMEM((1, heads), f32),
            pltpu.VMEM((1, heads), f32),
            dma((9,)),
            pltpu.VMEM((own_rows, gcols), half),
            pltpu.VMEM((nz, nx, ny, 2, own_rows, gcols), half),
            pltpu.VMEM((nz, nx, ny, 2, own_rows, cols), half),
            pltpu.VMEM((heads, seq, seq), half),
            pltpu.VMEM((groups, seq, heads // groups * seq), half),
            pltpu.VMEM((seq, cols), half),
            pltpu.VMEM((nz, nx, ny, 2, own_rows, seq), half),
            pltpu.VMEM((2 * nx, nz, ny, own_rows, seq), half),
            pltpu.VMEM((chunks, seq, CHUNK), f32),
            pltpu.VMEM((chunks, seq, CHUNK), half),
            pltpu.VMEM((chunks, seq, CHUNK), half),
            pltpu.VMEM((seq, cols), f32),
            pltpu.VMEM((groups, 2 * nx, seq, HEAD_DIM), half),
            pltpu.VMEM((groups, nz, ny, own_rows, HEAD_DIM), f32),
            pltpu.VMEM((groups, nz * ny, own_rows, HEAD_DIM), f32),
            pltpu.VMEM((nx * ny * 4, 1, 128), f32),
            pltpu.VMEM((nz, 1, 128), f32),
            dma, dma((nz * nx * ny,)), dma, dma, dma((nz * nx * ny,)), dma((nz,)),
            dma, dma((chunks,)), dma, dma, dma, dma((groups, 2 * nx)),
            dma, dma((groups,)), dma, dma, dma, dma,
        ],
        compiler_params=pltpu.CompilerParams(
            collective_id=0, has_side_effects=True, vmem_limit_bytes=60 * 1024 * 1024
        ),
    )(
        tokens, teacher, inner_weight, output_weight, state_weight.T, step_weight.T,
        step_bias[None, :], decay_log[None, :], skip_gain[None, :],
    )


def on_device(
    tokens,
    teacher,
    inner_weight,
    output_weight,
    inner_first,
    inner_second,
    state_weight,
    step_weight,
    step_bias,
    decay_log,
    skip_gain,
):
    loss, clipped = whole_step(
        tokens, teacher, inner_weight, output_weight, state_weight, step_weight,
        step_bias, decay_log, skip_gain,
    )
    first_fix = 1.0 - beta_one**STEP
    second_fix = 1.0 - beta_two**STEP
    first_next = beta_one * inner_first + (1.0 - beta_one) * clipped
    second_next = beta_two * inner_second + (1.0 - beta_two) * clipped * clipped
    update = (
        first_next / first_fix / (jnp.sqrt(second_next / second_fix) + adam_eps)
        + weight_decay * inner_weight
    )
    return (loss[0, 0], update, first_next, second_next)


def solution(mesh):
    finer = Mesh(
        mesh.devices.reshape(8, 4, 2, 2, mesh.shape["tensor"]),
        ("dp_0", "dp_1", "dp_2", "dp_3", "tensor"),
    )
    return jax.shard_map(
        on_device,
        mesh=finer,
        in_specs=(
            P(DP, None),
            P(DP, None),
            P(DP, "tensor"),
            P(DP, "tensor"),
            P(DP, "tensor"),
            P(DP, "tensor"),
            P(),
            P(None, "tensor"),
            P("tensor"),
            P("tensor"),
            P("tensor"),
        ),
        out_specs=(P(), P(DP, "tensor"), P(DP, "tensor"), P(DP, "tensor")),
        check_vma=False,
    )
```

```python
import functools
import heapq

import jax
import jax.numpy as jnp
from jax import lax
from jax.experimental import pallas as pl
from jax.experimental.pallas import tpu as pltpu
from jax.sharding import Mesh
from jax.sharding import PartitionSpec as P

HEAD_DIM = 128
STEP = 20
DP = ("dp_0", "dp_1", "dp_2", "dp_3")


beta_one = 0.9
beta_two = 0.95
adam_eps = 1e-08
weight_decay = 0.1
norm_eps = 1e-06


TORUS = ("dp_0", "dp_1", "dp_2")
BY_COLUMN = (("dp_2", "dp_1", "dp_0"), 2, False)
BY_ROW = (("dp_0", "dp_2", "dp_1"), 1, True)
CHUNK = 256
NARROW = 2
MIX_AT = 9.0


def ways(sizes):
    def sign(rel, order):
        n, v = sizes[order[2]], rel[order[2]]
        if 2 * v == n:
            return 1 if (rel[order[0]] + rel[order[1]]) % 2 == 0 else -1
        return 1 if 2 * v < n else -1

    def onward(rel, order):
        last = order[2]
        n = sizes[last]
        if rel[last] == 0:
            moves = [1, -1] if n > 2 else [1]
        else:
            moves = [sign(rel, order)]
        out = []
        for move in moves:
            nxt = dict(rel)
            nxt[last] = (rel[last] + move) % n
            far = nxt[last] if move > 0 else n - nxt[last]
            was = rel[last] if move > 0 else (n - rel[last]) % n
            if nxt[last] and far == was + 1 and (n == 2 or sign(nxt, order) == move):
                out.append(nxt)
        return out

    def children(rel, tree):
        order, straight, jump = tree
        last = order[2]
        if jump:
            out = [{**rel, last: v} for v in range(1, sizes[last])] if rel[last] == 0 else []
        else:
            out = onward(rel, order)
        zero = {a: 0 for a in TORUS}
        if not any(rel.values()):
            for i in range(sizes[order[0]]):
                for j in range(sizes[order[1]] if straight == 2 else 1):
                    if i or j:
                        out.append({**zero, order[0]: i, order[1]: j})
        if straight == 1 and rel[order[1]] == 0 and rel[order[2]] == 0:
            out += [{**rel, order[1]: j} for j in range(1, sizes[order[1]])]
        out.sort(key=lambda r: -sum(min(v, sizes[a] - v) for a, v in r.items()))
        return out

    return children


def relay_times(sizes, flows, latency=2.45, hop=0.45):
    children = ways(sizes)
    free, heap, count = {}, [], 0
    events = [[] for _ in flows]
    for n, (order, wire, start) in enumerate(flows):
        heapq.heappush(heap, (start, count, n, {a: 0 for a in TORUS}))
        count += 1
    while heap:
        now, _, n, rel = heapq.heappop(heap)
        order, wire, _ = flows[n]
        sends = children(rel, order)
        events[n].append((now, rel, sends))
        for nxt in sends:
            lands, hops = now, 0
            for a in TORUS:
                v = (nxt[a] - rel[a]) % sizes[a]
                if v:
                    go = 1 if 2 * v <= sizes[a] else -1
                    far = min(v, sizes[a] - v) * (2 if sizes[a] == 2 else 1)
                    begin = max(now, free.get((a, go), 0.0))
                    free[(a, go)] = begin + wire * far
                    lands = max(lands, begin + wire)
                    hops += far
            heapq.heappush(heap, (lands + latency + hop * (hops - 1) + (0.8 if n % 2 == 0 else 0.0), count, n, nxt))
            count += 1
    return events


def step_kernel(
    sizes,
    tokens_hbm, teacher_hbm, inner_weight_hbm, output_weight_hbm, state_weight_hbm,
    step_weight_hbm, step_bias_hbm, decay_log_hbm, skip_hbm,
    loss_out, clipped_out,
    tokens, teacher, inner_weight, output_weight, state_weight,
    step_weight, step_bias, decay_log, skip, load_sem, lend_send, lend_recv,
    mine, in_all, w_all, mix, mix_t, inner,
    tok_t, tok_all, part, leaving, arrived, arrived_wide, grad_acc, gp_all, g_part, g_half, g_all, row_a, row_b,
    in_send, in_recv, in_pair, w_send, w_recv, w_pair,
    student_send, student_recv, tok_send, tok_recv, gp_send, gp_recv,
    g_send, g_recv, a_send, a_recv, b_send, b_recv,
):
    axes = ("dp_0", "dp_1", "dp_2", "dp_3", "tensor")
    here = {a: lax.axis_index(a) for a in axes}
    nz, nx, ny = sizes["dp_0"], sizes["dp_1"], sizes["dp_2"]
    seq, features = tokens.shape
    cols = output_weight.shape[1]
    chunks = features // CHUNK
    heads = mix.shape[0]
    head_dim = cols // heads
    groups = inner_weight.shape[1] // head_dim
    per_group = heads // groups
    core = here["dp_3"]

    def ahead(a, v):
        return lax.rem(here[a] + (v % sizes[a]), sizes[a])

    def there(**by):
        return {a: ahead(a, v) for a, v in by.items() if v % sizes[a]}

    def remote(src, dst, send, recv, target):
        return pltpu.make_async_remote_copy(
            src, dst, send, recv, device_id=target, device_id_type=pl.DeviceIdType.MESH
        )

    plane = [
        dict(dp_1=i, dp_2=j, dp_3=k, tensor=t)
        for i in range(nx) for j in range(ny) for k in range(2) for t in range(2)
    ][1:]
    column = [dict(dp_0=i, dp_2=j) for i in range(nz) for j in range(ny)][1:]
    peers = plane + [dict(dp_0=i) for i in range(1, nz)]
    pair = there(dp_3=1)
    loads = [
        pltpu.make_async_copy(source, target, load_sem.at[n])
        for n, (source, target) in enumerate((
            (inner_weight_hbm, inner_weight), (output_weight_hbm, output_weight),
            (state_weight_hbm, state_weight), (step_weight_hbm, step_weight),
            (step_bias_hbm, step_bias), (decay_log_hbm, decay_log), (skip_hbm, skip),
            (tokens_hbm, tokens), (teacher_hbm, teacher),
        ))
    ]
    borrows = jnp.logical_and(core == 1, here["tensor"] == 1)
    lends = jnp.logical_and(core == 1, here["tensor"] == 0)
    lent = [
        remote(ref, ref, lend_send.at[n], lend_recv.at[n], there(tensor=1, dp_2=1))
        for n, ref in enumerate((tokens, teacher))
    ]
    for load in loads[:-2]:
        load.start()

    @pl.when(jnp.logical_not(borrows))
    def _():
        for load in loads[-2:]:
            load.start()

    barrier = pltpu.get_barrier_semaphore()
    for by in peers:
        pl.semaphore_signal(
            barrier, inc=1, device_id=there(**by), device_id_type=pl.DeviceIdType.MESH
        )
    for load in loads[:2]:
        load.wait()
    mine[...] = inner_weight[...].astype(jnp.bfloat16)
    in_all[here["dp_0"], here["dp_1"], here["dp_2"], core] = mine[...]
    w_all[here["dp_0"], here["dp_1"], here["dp_2"], core] = output_weight[...]

    in_wire, w_wire = 0.088, 0.352
    flows = (
        (BY_ROW, in_wire, 0.0), (BY_ROW, in_wire, 0.0),
        (BY_COLUMN, w_wire, 0.01), (BY_COLUMN, w_wire, 0.01),
    )
    events = relay_times(sizes, flows)
    steps = [
        sorted(
            [(t, 0, rel, sends) for t, rel, sends in events[c]]
            + [(t, 1, rel, sends) for t, rel, sends in events[2 + c]],
            key=lambda e: e[:2],
        )
        for c in range(2)
    ]

    def number(rel):
        return (rel["dp_0"] * nx + rel["dp_1"]) * ny + rel["dp_2"]

    def relay(c, begin, end):
        for time, kind, rel, sends in steps[c]:
            if not begin <= time < end:
                continue
            all_ref, own, send, recv = (
                (in_all, mine, in_send, in_recv), (w_all, output_weight, w_send, w_recv)
            )[kind]
            at = tuple(ahead(a, -rel[a]) for a in TORUS)
            slot = all_ref.at[at[0], at[1], at[2], c]
            first = not any(rel.values())
            block = own if first else slot
            if not first:
                remote(slot, slot, send, recv.at[number(rel)], pair).wait_recv()
            for nxt in sends:
                target = there(**{a: nxt[a] - rel[a] for a in TORUS})
                remote(block, slot, send, recv.at[number(nxt)], target).start()
            beside = in_pair if kind == 0 else w_pair.at[rel["dp_0"]]
            remote(block, slot, send, beside, pair).start()

    def relay_until(begin, end):
        for c in range(2):
            @pl.when(core == c)
            def _():
                relay(c, begin, end)

    def turn_tokens():
        per = tok_t.shape[4]
        rows_x = ny * 2 * per
        for k in range(features // 128):
            turned = tokens[:, k * 128 : (k + 1) * 128].T
            z, x = divmod(k * 128 // rows_x, nx)
            tok_t[z, x : x + 128 // rows_x] = turned.reshape(128 // rows_x, ny, 2, per, seq)

    def mix_heads():
        projected = lax.dot_general(
            tokens[...], state_weight[...], (((1,), (1,)), ((), ())),
            preferred_element_type=jnp.float32,
        )
        width = projected.shape[1] // 2
        b_coef, c_coef = projected[:, :width], projected[:, width:]
        gram = lax.dot_general(
            c_coef, b_coef, (((1,), (1,)), ((), ())),
            precision=lax.Precision.HIGHEST, preferred_element_type=jnp.float32,
        )
        raw = (
            lax.dot_general(
                tokens[...], step_weight[...], (((1,), (1,)), ((), ())),
                preferred_element_type=jnp.float32,
            )
            + step_bias[...]
        )
        step_size = jnp.maximum(raw, 0.0) + jnp.log1p(jnp.exp(-jnp.abs(raw)))
        rate = jnp.exp(decay_log[...]) * step_size
        later = lax.broadcasted_iota(jnp.int32, (seq, seq), 0)
        earlier = lax.broadcasted_iota(jnp.int32, (seq, seq), 1)
        causal = later >= earlier
        cumulative = jnp.dot(
            causal.astype(jnp.float32), rate,
            precision=lax.Precision.HIGHEST, preferred_element_type=jnp.float32,
        )
        blank = jnp.zeros((seq, seq - heads), jnp.float32)
        cum_t = jnp.concatenate([cumulative, blank], axis=1).T
        step_t = jnp.concatenate([step_size, blank], axis=1).T
        for h in range(heads):
            log_decay = cum_t[h : h + 1, :] - cumulative[:, h : h + 1]
            decay = jnp.where(causal, jnp.exp(jnp.minimum(log_decay, 0.0)), 0.0)
            mix[h] = (gram * decay * step_t[h : h + 1, :]).astype(jnp.bfloat16)

    def turn_mix():
        for g in range(groups):
            for h in range(per_group):
                mix_t[g, :, h * seq : (h + 1) * seq] = mix[g * per_group + h].T

    def project():
        width = inner_weight.shape[1]
        projected = jnp.dot(
            tokens[...], in_all[...].reshape(features, width),
            preferred_element_type=jnp.float32,
        ).astype(jnp.bfloat16)
        for g in range(groups):
            source = projected[:, g * head_dim : (g + 1) * head_dim]
            stack = mix[g * per_group : (g + 1) * per_group].reshape(per_group * seq, seq)
            mixed = jnp.dot(stack, source, preferred_element_type=jnp.float32)
            wide = source.astype(jnp.float32)
            for h in range(per_group):
                n = g * per_group + h
                inner[:, n * head_dim : (n + 1) * head_dim] = (
                    mixed[h * seq : (h + 1) * seq] + skip[:, n : n + 1] * wide
                ).astype(jnp.bfloat16)

    other_half = {"tensor": 1 - here["tensor"], "dp_2": lax.rem(here["dp_2"] + core, ny)}
    order = sorted(range(nz), key=lambda v: (min(v, nz - v), v))

    wide = chunks - leaving.shape[0]

    def student_copy(i):
        source, target = (part, arrived_wide) if i < wide else (leaving, arrived)
        at = i if i < wide else i - wide
        return remote(
            source.at[at], target.at[at], student_send.at[int(i < wide)],
            student_recv.at[i], other_half,
        )

    def came(i):
        return arrived_wide[i] if i < wide else arrived[i - wide].astype(jnp.float32)

    def w_rows(i):
        return w_all[ahead("dp_0", -order[i])].reshape(CHUNK, cols)

    def teacher_cols(i):
        return teacher[:, pl.ds(pl.multiple_of(ahead("dp_0", -order[i]) * CHUNK, CHUNK), CHUNK)]

    def student(i):
        beside = w_all.at[0, :, :, 0]
        remote(beside, beside, w_send, w_pair.at[order[i]], pair).wait_recv()
        piece = lax.dot_general(
            inner[...], w_rows(i), (((1,), (1,)), ((), ())), preferred_element_type=jnp.float32
        )
        part[i] = piece
        if i >= wide:
            leaving[i - wide] = piece.astype(jnp.bfloat16)
        if i:
            student_copy(i - 1).start()

    pl.semaphore_wait(barrier, len(peers))
    late = max(t for t, *_ in steps[0] + steps[1]) + 1
    inner_done = max(t for c in range(2) for t, kind, *_ in steps[c] if kind == 0) + 1e-6
    @pl.when(jnp.logical_not(borrows))
    def _():
        for load in loads[-2:]:
            load.wait()

    @pl.when(lends)
    def _():
        for copy in lent:
            copy.start()

    relay_until(0, 2.0)
    for load in loads[2:-2]:
        load.wait()
    relay_until(2.0, MIX_AT)

    @pl.when(borrows)
    def _():
        lent[0].wait_recv()

    turn_tokens()
    mix_heads()
    turn_mix()
    relay_until(MIX_AT, max(inner_done, MIX_AT))
    beside = in_all.at[:, :, :, 0]
    remote(beside, beside, in_send, in_pair, pair).wait_recv()
    project()
    tok_sends = []
    for i in range(nx):
        for k in range(2):
            slot = i * 2 + k
            to_x = lax.rem(here["dp_1"] + i, nx)
            to_c = lax.rem(here["dp_3"] + k, 2)
            if slot:
                tok_sends.append((slot, to_x, to_c, there(dp_1=i, dp_3=k)))
    for slot, to_x, to_c, target in tok_sends:
        remote(
            tok_t.at[:, to_x, :, to_c], tok_all.at[slot], tok_send, tok_recv, target
        ).start()
    tok_all[0] = tok_t[:, here["dp_1"], :, here["dp_3"]]

    reached = max(inner_done, MIX_AT)
    for i in range(chunks):
        needed = max(
            t for c in range(2) for t, kind, rel, _ in steps[c]
            if kind == 1 and rel["dp_0"] == order[i]
        ) + 1e-6
        if needed > reached:
            relay_until(reached, needed)
            reached = needed
        student(i)
    relay_until(reached, late)
    student_copy(chunks - 1).start()

    @pl.when(borrows)
    def _():
        lent[1].wait_recv()

    @pl.when(lends)
    def _():
        for copy in lent:
            copy.wait_send()

    squares = jnp.zeros((8, CHUNK), jnp.float32)
    for i in range(chunks):
        student_copy(i).wait_recv()
        error = (
            part[i] + came(i)
            - teacher_cols(i).astype(jnp.float32)
        )
        squares = squares + jnp.sum((error * error).reshape(seq // 8, 8, CHUNK), axis=0)
        product = jnp.dot(
            error.astype(jnp.bfloat16), w_rows(i), preferred_element_type=jnp.float32,
        )
        if i == 0:
            grad_acc[...] = product
        else:
            grad_acc[...] += product
    near = (1, 3, 2) if nx == 4 else range(1, nx)
    members = 2 * nx

    def gp_copy(g, source, slot, target):
        return remote(
            gp_all.at[g, source], gp_all.at[g, slot], gp_send, gp_recv.at[g, slot], target
        )

    for g in range(groups):
        heads_here = []
        direct = None
        for h in range(per_group):
            n = g * per_group + h
            one = grad_acc[:, n * head_dim : (n + 1) * head_dim].astype(jnp.bfloat16)
            heads_here.append(one)
            term = skip[:, n : n + 1] * one.astype(jnp.float32)
            direct = term if direct is None else direct + term
        back = jnp.dot(
            mix_t[g], jnp.concatenate(heads_here, axis=0), preferred_element_type=jnp.float32
        )
        gp_all[g, 0] = (back + direct).astype(jnp.bfloat16)
        for i in reversed(near):
            gp_copy(g, 0, 2 * i, there(dp_1=i)).start()
        gp_copy(g, 0, 1, pair).start()
    remote(
        tok_all.at[pl.ds(1, members - 1)], tok_all.at[pl.ds(1, members - 1)],
        tok_send, tok_recv, pair,
    ).wait()

    def product_of(g, slot):
        left = tok_all[slot].reshape(-1, seq)
        return jnp.dot(left, gp_all[g, slot], preferred_element_type=jnp.float32)

    outward = sorted(column, key=lambda b: -min(b["dp_0"], nz - b["dp_0"]) - b["dp_2"])
    for g in range(groups):
        gp_copy(g, 1, 1, pair).wait_recv()
        total = product_of(g, 0) + product_of(g, 1)
        for i in near:
            gp_copy(g, 0, 2 * i, pair).wait_recv()
            gp_copy(g, 2 * i, 2 * i + 1, pair).start()
            total = total + product_of(g, 2 * i)
        for i in near:
            gp_copy(g, 0, 2 * i + 1, pair).wait_recv()
            total = total + product_of(g, 2 * i + 1)
        g_half[g] = total.reshape(g_part.shape[1:]).astype(jnp.bfloat16)
        g_part[g] = total.reshape(g_part.shape[1:])
        for by in outward:
            slot = by["dp_0"] * ny + by["dp_2"]
            to_z, to_y = ahead("dp_0", by["dp_0"]), ahead("dp_2", by["dp_2"])
            remote(
                g_half.at[g, to_z, to_y], g_all.at[g, slot], g_send, g_recv.at[g], there(**by)
            ).start()
    err = jnp.sum(squares) * 0.5
    halves = []
    for g in range(groups):
        rest = g_all.at[g, pl.ds(1, nz * ny - 1)]
        remote(rest, rest, g_send, g_recv.at[g], pair).wait_recv()
        halves.append(
            g_part[g, here["dp_0"], here["dp_2"]]
            + jnp.sum(g_all[g, 1:].astype(jnp.float32), axis=0)
        )
    grad = jnp.concatenate(halves, axis=1)
    lane = lax.broadcasted_iota(jnp.int32, (1, 128), 1)
    row = jnp.where(lane == 0, jnp.sum(grad * grad), jnp.where(lane == 1, err, 0.0))
    row_a[0] = row
    for n, by in enumerate(plane):
        remote(row_a.at[0], row_a.at[n + 1], a_send, a_recv, there(**by)).start()
    rest = row_a.at[pl.ds(1, len(plane))]
    remote(rest, rest, a_send, a_recv, pair).wait()
    row_b[0] = jnp.sum(row_a[...], axis=0)
    for i in range(1, nz):
        remote(row_b.at[0], row_b.at[i], b_send, b_recv, there(dp_0=i)).start()
    rest = row_b.at[pl.ds(1, nz - 1)]
    remote(rest, rest, b_send, b_recv, pair).wait()
    sums = jnp.sum(row_b[...], axis=0)
    root_mean = jnp.sqrt(sums[:, 0:1] / (features * inner_weight.shape[1] * 2))
    factor = jnp.minimum(1.0, 1.0 / (root_mean + norm_eps))
    loss_out[...] = jnp.broadcast_to(sums[:, 1:2] / (nz * nx * ny * 2 * seq * features), (1, 128))
    clipped_out[...] = factor * grad
    for g in range(groups):
        rest = gp_all.at[g, pl.ds(1, members - 1)]
        remote(rest, rest, gp_send, gp_recv.at[g, 1], pair).wait_send()
        rest = g_all.at[g, pl.ds(1, nz * ny - 1)]
        remote(rest, rest, g_send, g_recv.at[g], pair).wait_send()
    remote(leaving, leaving, student_send.at[0], student_recv.at[0], pair).wait_send()
    remote(arrived_wide, arrived_wide, student_send.at[1], student_recv.at[0], pair).wait_send()
    pieces = nz * nx * ny
    for block, ref, send in (((0,), in_all, in_send), ((0,), w_all, w_send)):
        half = ref.at[:, :, :, 0]
        remote(half, half, send, in_pair, pair).wait_send()
        rest = ref.at[pl.ds(0, nz - 1), :, :, 0]
        remote(rest, rest, send, in_pair, pair).wait_send()
        rest = ref.at[0, pl.ds(0, nx - 1), :, 0]
        remote(rest, rest, send, in_pair, pair).wait_send()
        rest = ref.at[0, 0, pl.ds(0, ny - 1), 0]
        remote(rest, rest, send, in_pair, pair).wait_send()


def whole_step(
    tokens, teacher, inner_weight, output_weight, state_weight, step_weight,
    step_bias, decay_log, skip_gain,
):
    sizes = {a: lax.axis_size(a) for a in ("dp_0", "dp_1", "dp_2", "dp_3", "tensor")}
    nz, nx, ny = sizes["dp_0"], sizes["dp_1"], sizes["dp_2"]
    seq, features = tokens.shape
    own_rows, cols = output_weight.shape
    gcols = inner_weight.shape[1]
    heads = step_weight.shape[1]
    chunks = features // CHUNK
    groups = gcols // HEAD_DIM
    f32, half = jnp.float32, jnp.bfloat16
    vmem = pl.BlockSpec(memory_space=pltpu.VMEM)
    dma = pltpu.SemaphoreType.DMA
    return pl.pallas_call(
        functools.partial(step_kernel, sizes),
        name="whole_step",
        out_shape=(
            jax.ShapeDtypeStruct((1, 128), f32),
            jax.ShapeDtypeStruct((own_rows, gcols), f32),
        ),
        in_specs=[pl.BlockSpec(memory_space=pl.ANY)] * 9,
        out_specs=(vmem,) * 2,
        scratch_shapes=[
            pltpu.VMEM((seq, features), half),
            pltpu.VMEM((seq, features), half),
            pltpu.VMEM((own_rows, gcols), f32),
            pltpu.VMEM((own_rows, cols), half),
            pltpu.VMEM((state_weight.shape[1], features), half),
            pltpu.VMEM((heads, features), half),
            pltpu.VMEM((1, heads), f32),
            pltpu.VMEM((1, heads), f32),
            pltpu.VMEM((1, heads), f32),
            dma((9,)),
            dma((2,)),
            dma((2,)),
            pltpu.VMEM((own_rows, gcols), half),
            pltpu.VMEM((nz, nx, ny, 2, own_rows, gcols), half),
            pltpu.VMEM((nz, nx, ny, 2, own_rows, cols), half),
            pltpu.VMEM((heads, seq, seq), half),
            pltpu.VMEM((groups, seq, heads // groups * seq), half),
            pltpu.VMEM((seq, cols), half),
            pltpu.VMEM((nz, nx, ny, 2, own_rows, seq), half),
            pltpu.VMEM((2 * nx, nz, ny, own_rows, seq), half),
            pltpu.VMEM((chunks, seq, CHUNK), f32),
            pltpu.VMEM((NARROW, seq, CHUNK), half),
            pltpu.VMEM((NARROW, seq, CHUNK), half),
            pltpu.VMEM((chunks - NARROW, seq, CHUNK), f32),
            pltpu.VMEM((seq, cols), f32),
            pltpu.VMEM((groups, 2 * nx, seq, HEAD_DIM), half),
            pltpu.VMEM((groups, nz, ny, own_rows, HEAD_DIM), f32),
            pltpu.VMEM((groups, nz, ny, own_rows, HEAD_DIM), half),
            pltpu.VMEM((groups, nz * ny, own_rows, HEAD_DIM), half),
            pltpu.VMEM((nx * ny * 4, 1, 128), f32),
            pltpu.VMEM((nz, 1, 128), f32),
            dma, dma((nz * nx * ny,)), dma, dma, dma((nz * nx * ny,)), dma((nz,)),
            dma((2,)), dma((chunks,)), dma, dma, dma, dma((groups, 2 * nx)),
            dma, dma((groups,)), dma, dma, dma, dma,
        ],
        compiler_params=pltpu.CompilerParams(
            collective_id=0, has_side_effects=True, vmem_limit_bytes=60 * 1024 * 1024
        ),
    )(
        tokens, teacher, inner_weight, output_weight, state_weight.T, step_weight.T,
        step_bias[None, :], decay_log[None, :], skip_gain[None, :],
    )


def on_device(
    tokens,
    teacher,
    inner_weight,
    output_weight,
    inner_first,
    inner_second,
    state_weight,
    step_weight,
    step_bias,
    decay_log,
    skip_gain,
):
    loss, clipped = whole_step(
        tokens, teacher, inner_weight, output_weight, state_weight, step_weight,
        step_bias, decay_log, skip_gain,
    )
    first_fix = 1.0 - beta_one**STEP
    second_fix = 1.0 - beta_two**STEP
    first_next = beta_one * inner_first + (1.0 - beta_one) * clipped
    second_next = beta_two * inner_second + (1.0 - beta_two) * clipped * clipped
    update = (
        first_next / first_fix / (jnp.sqrt(second_next / second_fix) + adam_eps)
        + weight_decay * inner_weight
    )
    return (loss[0, 0], update, first_next, second_next)


def solution(mesh):
    finer = Mesh(
        mesh.devices.reshape(8, 4, 2, 2, mesh.shape["tensor"]),
        ("dp_0", "dp_1", "dp_2", "dp_3", "tensor"),
    )
    return jax.shard_map(
        on_device,
        mesh=finer,
        in_specs=(
            P(DP, None),
            P(DP, None),
            P(DP, "tensor"),
            P(DP, "tensor"),
            P(DP, "tensor"),
            P(DP, "tensor"),
            P(),
            P(None, "tensor"),
            P("tensor"),
            P("tensor"),
            P("tensor"),
        ),
        out_specs=(P(), P(DP, "tensor"), P(DP, "tensor"), P(DP, "tensor")),
        check_vma=False,
    )
```

```python
import functools
import heapq

import jax
import jax.numpy as jnp
from jax import lax
from jax.experimental import pallas as pl
from jax.experimental.pallas import tpu as pltpu
from jax.sharding import Mesh
from jax.sharding import PartitionSpec as P

HEAD_DIM = 128
STEP = 20
DP = ("dp_0", "dp_1", "dp_2", "dp_3")


beta_one = 0.9
beta_two = 0.95
adam_eps = 1e-08
weight_decay = 0.1
norm_eps = 1e-06


TORUS = ("dp_0", "dp_1", "dp_2")
BY_COLUMN = (("dp_2", "dp_1", "dp_0"), 2, False)
BY_ROW = (("dp_0", "dp_2", "dp_1"), 1, True)
CHUNK = 256
NARROW = 3
MIX_AT = 9.0


def ways(sizes):
    def sign(rel, order):
        n, v = sizes[order[2]], rel[order[2]]
        if 2 * v == n:
            return 1 if (rel[order[0]] + rel[order[1]]) % 2 == 0 else -1
        return 1 if 2 * v < n else -1

    def onward(rel, order):
        last = order[2]
        n = sizes[last]
        if rel[last] == 0:
            moves = [1, -1] if n > 2 else [1]
        else:
            moves = [sign(rel, order)]
        out = []
        for move in moves:
            nxt = dict(rel)
            nxt[last] = (rel[last] + move) % n
            far = nxt[last] if move > 0 else n - nxt[last]
            was = rel[last] if move > 0 else (n - rel[last]) % n
            if nxt[last] and far == was + 1 and (n == 2 or sign(nxt, order) == move):
                out.append(nxt)
        return out

    def children(rel, tree):
        order, straight, jump = tree
        last = order[2]
        if jump:
            out = [{**rel, last: v} for v in range(1, sizes[last])] if rel[last] == 0 else []
        else:
            out = onward(rel, order)
        zero = {a: 0 for a in TORUS}
        if not any(rel.values()):
            for i in range(sizes[order[0]]):
                for j in range(sizes[order[1]] if straight == 2 else 1):
                    if i or j:
                        out.append({**zero, order[0]: i, order[1]: j})
        if straight == 1 and rel[order[1]] == 0 and rel[order[2]] == 0:
            out += [{**rel, order[1]: j} for j in range(1, sizes[order[1]])]
        out.sort(key=lambda r: -sum(min(v, sizes[a] - v) for a, v in r.items()))
        return out

    return children


def relay_times(sizes, flows, latency=2.6, hop=0.45):
    children = ways(sizes)
    free, heap, count = {}, [], 0
    events = [[] for _ in flows]
    for n, (order, wire, start) in enumerate(flows):
        heapq.heappush(heap, (start, count, n, {a: 0 for a in TORUS}))
        count += 1
    while heap:
        now, _, n, rel = heapq.heappop(heap)
        order, wire, _ = flows[n]
        sends = children(rel, order)
        events[n].append((now, rel, sends))
        for nxt in sends:
            lands, hops = now, 0
            for a in TORUS:
                v = (nxt[a] - rel[a]) % sizes[a]
                if v:
                    go = 1 if 2 * v <= sizes[a] else -1
                    far = min(v, sizes[a] - v) * (2 if sizes[a] == 2 else 1)
                    begin = max(now, free.get((a, go), 0.0))
                    free[(a, go)] = begin + wire * far
                    lands = max(lands, begin + wire)
                    hops += far
            heapq.heappush(heap, (lands + latency + hop * (hops - 1) + (1.0 if n % 2 == 0 else 0.0), count, n, nxt))
            count += 1
    return events


def step_kernel(
    sizes,
    tokens_hbm, teacher_hbm, inner_weight_hbm, output_weight_hbm, state_weight_hbm,
    step_weight_hbm, step_bias_hbm, decay_log_hbm, skip_hbm,
    loss_out, clipped_out,
    tokens, teacher, inner_weight, output_weight, state_weight,
    step_weight, step_bias, decay_log, skip, load_sem, lend_send, lend_recv,
    mine, in_all, w_all, mix, mix_t, inner,
    tok_t, tok_all, part, leaving, arrived, arrived_wide, grad_acc, gp_all, g_part, g_half, g_all, row_a, row_b,
    in_send, in_recv, in_pair, w_send, w_recv, w_pair,
    student_send, student_recv, tok_send, tok_recv, gp_send, gp_recv,
    g_send, g_recv, a_send, a_recv, b_send, b_recv,
):
    axes = ("dp_0", "dp_1", "dp_2", "dp_3", "tensor")
    here = {a: lax.axis_index(a) for a in axes}
    nz, nx, ny = sizes["dp_0"], sizes["dp_1"], sizes["dp_2"]
    seq, features = tokens.shape
    cols = output_weight.shape[1]
    chunks = features // CHUNK
    heads = mix.shape[0]
    head_dim = cols // heads
    groups = inner_weight.shape[1] // head_dim
    per_group = heads // groups
    core = here["dp_3"]

    def ahead(a, v):
        return lax.rem(here[a] + (v % sizes[a]), sizes[a])

    def there(**by):
        return {a: ahead(a, v) for a, v in by.items() if v % sizes[a]}

    def remote(src, dst, send, recv, target):
        return pltpu.make_async_remote_copy(
            src, dst, send, recv, device_id=target, device_id_type=pl.DeviceIdType.MESH
        )

    plane = [
        dict(dp_1=i, dp_2=j, dp_3=k, tensor=t)
        for i in range(nx) for j in range(ny) for k in range(2) for t in range(2)
    ][1:]
    column = [dict(dp_0=i, dp_2=j) for i in range(nz) for j in range(ny)][1:]
    peers = plane + [dict(dp_0=i) for i in range(1, nz)]
    pair = there(dp_3=1)
    loads = [
        pltpu.make_async_copy(source, target, load_sem.at[n])
        for n, (source, target) in enumerate((
            (inner_weight_hbm, inner_weight), (output_weight_hbm, output_weight),
            (state_weight_hbm, state_weight), (step_weight_hbm, step_weight),
            (step_bias_hbm, step_bias), (decay_log_hbm, decay_log), (skip_hbm, skip),
            (tokens_hbm, tokens), (teacher_hbm, teacher),
        ))
    ]
    borrows = jnp.logical_and(core == 1, here["tensor"] == 1)
    lends = jnp.logical_and(core == 1, here["tensor"] == 0)
    lent = [
        remote(ref, ref, lend_send.at[n], lend_recv.at[n], there(tensor=1, dp_2=1))
        for n, ref in enumerate((tokens, teacher))
    ]
    for load in loads[:-2]:
        load.start()

    @pl.when(jnp.logical_not(borrows))
    def _():
        for load in loads[-2:]:
            load.start()

    barrier = pltpu.get_barrier_semaphore()
    for by in peers:
        pl.semaphore_signal(
            barrier, inc=1, device_id=there(**by), device_id_type=pl.DeviceIdType.MESH
        )
    for load in loads[:2]:
        load.wait()
    mine[...] = inner_weight[...].astype(jnp.bfloat16)
    in_all[here["dp_0"], here["dp_1"], here["dp_2"], core] = mine[...]
    w_all[here["dp_0"], here["dp_1"], here["dp_2"], core] = output_weight[...]

    in_wire, w_wire = 0.088, 0.352
    flows = (
        (BY_ROW, in_wire, 0.0), (BY_ROW, in_wire, 0.0),
        (BY_COLUMN, w_wire, -0.01), (BY_COLUMN, w_wire, -0.01),
    )
    events = relay_times(sizes, flows)
    steps = [
        sorted(
            [(t, 0, rel, sends) for t, rel, sends in events[c]]
            + [(t, 1, rel, sends) for t, rel, sends in events[2 + c]],
            key=lambda e: e[:2],
        )
        for c in range(2)
    ]

    def number(rel):
        return (rel["dp_0"] * nx + rel["dp_1"]) * ny + rel["dp_2"]

    def relay(c, begin, end):
        for time, kind, rel, sends in steps[c]:
            if not begin <= time < end:
                continue
            all_ref, own, send, recv = (
                (in_all, mine, in_send, in_recv), (w_all, output_weight, w_send, w_recv)
            )[kind]
            at = tuple(ahead(a, -rel[a]) for a in TORUS)
            slot = all_ref.at[at[0], at[1], at[2], c]
            first = not any(rel.values())
            block = own if first else slot
            if not first:
                remote(slot, slot, send, recv.at[number(rel)], pair).wait_recv()
            for nxt in sends:
                target = there(**{a: nxt[a] - rel[a] for a in TORUS})
                remote(block, slot, send, recv.at[number(nxt)], target).start()
            beside = in_pair if kind == 0 else w_pair.at[rel["dp_0"]]
            remote(block, slot, send, beside, pair).start()

    def relay_until(begin, end):
        for c in range(2):
            @pl.when(core == c)
            def _():
                relay(c, begin, end)

    def turn_tokens():
        per = tok_t.shape[4]
        rows_x = ny * 2 * per
        for k in range(features // 128):
            turned = tokens[:, k * 128 : (k + 1) * 128].T
            z, x = divmod(k * 128 // rows_x, nx)
            tok_t[z, x : x + 128 // rows_x] = turned.reshape(128 // rows_x, ny, 2, per, seq)

    def mix_heads():
        projected = lax.dot_general(
            tokens[...], state_weight[...], (((1,), (1,)), ((), ())),
            preferred_element_type=jnp.float32,
        )
        width = projected.shape[1] // 2
        b_coef, c_coef = projected[:, :width], projected[:, width:]
        gram = lax.dot_general(
            c_coef, b_coef, (((1,), (1,)), ((), ())),
            precision=lax.Precision.HIGHEST, preferred_element_type=jnp.float32,
        )
        raw = (
            lax.dot_general(
                tokens[...], step_weight[...], (((1,), (1,)), ((), ())),
                preferred_element_type=jnp.float32,
            )
            + step_bias[...]
        )
        step_size = jnp.maximum(raw, 0.0) + jnp.log1p(jnp.exp(-jnp.abs(raw)))
        rate = jnp.exp(decay_log[...]) * step_size
        later = lax.broadcasted_iota(jnp.int32, (seq, seq), 0)
        earlier = lax.broadcasted_iota(jnp.int32, (seq, seq), 1)
        causal = later >= earlier
        cumulative = jnp.dot(
            causal.astype(jnp.float32), rate,
            precision=lax.Precision.HIGHEST, preferred_element_type=jnp.float32,
        )
        blank = jnp.zeros((seq, seq - heads), jnp.float32)
        cum_t = jnp.concatenate([cumulative, blank], axis=1).T
        step_t = jnp.concatenate([step_size, blank], axis=1).T
        for h in range(heads):
            log_decay = cum_t[h : h + 1, :] - cumulative[:, h : h + 1]
            decay = jnp.where(causal, jnp.exp(jnp.minimum(log_decay, 0.0)), 0.0)
            mix[h] = (gram * decay * step_t[h : h + 1, :]).astype(jnp.bfloat16)

    def turn_mix():
        for g in range(groups):
            for h in range(per_group):
                mix_t[g, :, h * seq : (h + 1) * seq] = mix[g * per_group + h].T

    def project():
        width = inner_weight.shape[1]
        projected = jnp.dot(
            tokens[...], in_all[...].reshape(features, width),
            preferred_element_type=jnp.float32,
        ).astype(jnp.bfloat16)
        for g in range(groups):
            source = projected[:, g * head_dim : (g + 1) * head_dim]
            stack = mix[g * per_group : (g + 1) * per_group].reshape(per_group * seq, seq)
            mixed = jnp.dot(stack, source, preferred_element_type=jnp.float32)
            wide = source.astype(jnp.float32)
            for h in range(per_group):
                n = g * per_group + h
                inner[:, n * head_dim : (n + 1) * head_dim] = (
                    mixed[h * seq : (h + 1) * seq] + skip[:, n : n + 1] * wide
                ).astype(jnp.bfloat16)

    other_half = {"tensor": 1 - here["tensor"], "dp_2": lax.rem(here["dp_2"] + core, ny)}
    order = sorted(range(nz), key=lambda v: (min(v, nz - v), v))

    wide = chunks - leaving.shape[0]

    def student_copy(i):
        source, target = (part, arrived_wide) if i < wide else (leaving, arrived)
        at = i if i < wide else i - wide
        return remote(
            source.at[at], target.at[at], student_send.at[int(i < wide)],
            student_recv.at[i], other_half,
        )

    def came(i):
        return arrived_wide[i] if i < wide else arrived[i - wide].astype(jnp.float32)

    def w_rows(i):
        return w_all[ahead("dp_0", -order[i])].reshape(CHUNK, cols)

    def teacher_cols(i):
        return teacher[:, pl.ds(pl.multiple_of(ahead("dp_0", -order[i]) * CHUNK, CHUNK), CHUNK)]

    def student(i):
        beside = w_all.at[0, :, :, 0]
        remote(beside, beside, w_send, w_pair.at[order[i]], pair).wait_recv()
        piece = lax.dot_general(
            inner[...], w_rows(i), (((1,), (1,)), ((), ())), preferred_element_type=jnp.float32
        )
        part[i] = piece
        if i >= wide:
            leaving[i - wide] = piece.astype(jnp.bfloat16)
        if i:
            student_copy(i - 1).start()

    pl.semaphore_wait(barrier, len(peers))
    late = max(t for t, *_ in steps[0] + steps[1]) + 1
    inner_done = max(t for c in range(2) for t, kind, *_ in steps[c] if kind == 0) + 1e-6
    @pl.when(jnp.logical_not(borrows))
    def _():
        for load in loads[-2:]:
            load.wait()

    @pl.when(lends)
    def _():
        for copy in lent:
            copy.start()

    relay_until(-1.0, 2.0)
    for load in loads[2:-2]:
        load.wait()
    relay_until(2.0, MIX_AT)

    @pl.when(borrows)
    def _():
        lent[0].wait_recv()

    turn_tokens()
    mix_heads()
    turn_mix()
    relay_until(MIX_AT, max(inner_done, MIX_AT))
    beside = in_all.at[:, :, :, 0]
    remote(beside, beside, in_send, in_pair, pair).wait_recv()
    project()
    tok_sends = []
    for i in range(nx):
        for k in range(2):
            slot = i * 2 + k
            to_x = lax.rem(here["dp_1"] + i, nx)
            to_c = lax.rem(here["dp_3"] + k, 2)
            if slot:
                tok_sends.append((slot, to_x, to_c, there(dp_1=i, dp_3=k)))
    for slot, to_x, to_c, target in tok_sends:
        remote(
            tok_t.at[:, to_x, :, to_c], tok_all.at[slot], tok_send, tok_recv, target
        ).start()
    tok_all[0] = tok_t[:, here["dp_1"], :, here["dp_3"]]

    reached = max(inner_done, MIX_AT)
    for i in range(chunks):
        needed = max(
            t for c in range(2) for t, kind, rel, _ in steps[c]
            if kind == 1 and rel["dp_0"] == order[i]
        ) + 1e-6
        if needed > reached:
            relay_until(reached, needed)
            reached = needed
        student(i)
    relay_until(reached, late)
    student_copy(chunks - 1).start()

    @pl.when(borrows)
    def _():
        lent[1].wait_recv()

    @pl.when(lends)
    def _():
        for copy in lent:
            copy.wait_send()

    squares = jnp.zeros((8, CHUNK), jnp.float32)
    for i in range(chunks):
        student_copy(i).wait_recv()
        error = (
            part[i] + came(i)
            - teacher_cols(i).astype(jnp.float32)
        )
        squares = squares + jnp.sum((error * error).reshape(seq // 8, 8, CHUNK), axis=0)
        product = jnp.dot(
            error.astype(jnp.bfloat16), w_rows(i), preferred_element_type=jnp.float32,
        )
        if i == 0:
            grad_acc[...] = product
        else:
            grad_acc[...] += product
    near = (1, 3, 2) if nx == 4 else range(1, nx)
    members = 2 * nx

    def gp_copy(g, source, slot, target):
        return remote(
            gp_all.at[g, source], gp_all.at[g, slot], gp_send, gp_recv.at[g, slot], target
        )

    for g in range(groups):
        heads_here = []
        direct = None
        for h in range(per_group):
            n = g * per_group + h
            one = grad_acc[:, n * head_dim : (n + 1) * head_dim].astype(jnp.bfloat16)
            heads_here.append(one)
            term = skip[:, n : n + 1] * one.astype(jnp.float32)
            direct = term if direct is None else direct + term
        back = jnp.dot(
            mix_t[g], jnp.concatenate(heads_here, axis=0), preferred_element_type=jnp.float32
        )
        gp_all[g, 0] = (back + direct).astype(jnp.bfloat16)
        for i in reversed(near):
            gp_copy(g, 0, 2 * i, there(dp_1=i)).start()
        gp_copy(g, 0, 1, pair).start()
    remote(
        tok_all.at[pl.ds(1, members - 1)], tok_all.at[pl.ds(1, members - 1)],
        tok_send, tok_recv, pair,
    ).wait()

    def product_of(g, slot):
        left = tok_all[slot].reshape(-1, seq)
        return jnp.dot(left, gp_all[g, slot], preferred_element_type=jnp.float32)

    outward = sorted(column, key=lambda b: -min(b["dp_0"], nz - b["dp_0"]) - b["dp_2"])
    for g in range(groups):
        gp_copy(g, 1, 1, pair).wait_recv()
        total = product_of(g, 0) + product_of(g, 1)
        for i in near:
            gp_copy(g, 0, 2 * i, pair).wait_recv()
            gp_copy(g, 2 * i, 2 * i + 1, pair).start()
            total = total + product_of(g, 2 * i)
        for i in near:
            gp_copy(g, 0, 2 * i + 1, pair).wait_recv()
            total = total + product_of(g, 2 * i + 1)
        g_half[g] = total.reshape(g_part.shape[1:]).astype(jnp.bfloat16)
        g_part[g] = total.reshape(g_part.shape[1:])
        for by in outward:
            slot = by["dp_0"] * ny + by["dp_2"]
            to_z, to_y = ahead("dp_0", by["dp_0"]), ahead("dp_2", by["dp_2"])
            remote(
                g_half.at[g, to_z, to_y], g_all.at[g, slot], g_send, g_recv.at[g], there(**by)
            ).start()
    err = jnp.sum(squares) * 0.5
    halves = []
    for g in range(groups):
        rest = g_all.at[g, pl.ds(1, nz * ny - 1)]
        remote(rest, rest, g_send, g_recv.at[g], pair).wait_recv()
        halves.append(
            g_part[g, here["dp_0"], here["dp_2"]]
            + jnp.sum(g_all[g, 1:].astype(jnp.float32), axis=0)
        )
    grad = jnp.concatenate(halves, axis=1)
    lane = lax.broadcasted_iota(jnp.int32, (1, 128), 1)
    row = jnp.where(lane == 0, jnp.sum(grad * grad), jnp.where(lane == 1, err, 0.0))
    row_a[0] = row
    for n, by in enumerate(plane):
        remote(row_a.at[0], row_a.at[n + 1], a_send, a_recv, there(**by)).start()
    rest = row_a.at[pl.ds(1, len(plane))]
    remote(rest, rest, a_send, a_recv, pair).wait()
    row_b[0] = jnp.sum(row_a[...], axis=0)
    for i in range(1, nz):
        remote(row_b.at[0], row_b.at[i], b_send, b_recv, there(dp_0=i)).start()
    rest = row_b.at[pl.ds(1, nz - 1)]
    remote(rest, rest, b_send, b_recv, pair).wait()
    sums = jnp.sum(row_b[...], axis=0)
    root_mean = jnp.sqrt(sums[:, 0:1] / (features * inner_weight.shape[1] * 2))
    factor = jnp.minimum(1.0, 1.0 / (root_mean + norm_eps))
    loss_out[...] = jnp.broadcast_to(sums[:, 1:2] / (nz * nx * ny * 2 * seq * features), (1, 128))
    clipped_out[...] = factor * grad
    for g in range(groups):
        rest = gp_all.at[g, pl.ds(1, members - 1)]
        remote(rest, rest, gp_send, gp_recv.at[g, 1], pair).wait_send()
        rest = g_all.at[g, pl.ds(1, nz * ny - 1)]
        remote(rest, rest, g_send, g_recv.at[g], pair).wait_send()
    remote(leaving, leaving, student_send.at[0], student_recv.at[0], pair).wait_send()
    remote(arrived_wide, arrived_wide, student_send.at[1], student_recv.at[0], pair).wait_send()
    pieces = nz * nx * ny
    for block, ref, send in (((0,), in_all, in_send), ((0,), w_all, w_send)):
        half = ref.at[:, :, :, 0]
        remote(half, half, send, in_pair, pair).wait_send()
        rest = ref.at[pl.ds(0, nz - 1), :, :, 0]
        remote(rest, rest, send, in_pair, pair).wait_send()
        rest = ref.at[0, pl.ds(0, nx - 1), :, 0]
        remote(rest, rest, send, in_pair, pair).wait_send()
        rest = ref.at[0, 0, pl.ds(0, ny - 1), 0]
        remote(rest, rest, send, in_pair, pair).wait_send()


def whole_step(
    tokens, teacher, inner_weight, output_weight, state_weight, step_weight,
    step_bias, decay_log, skip_gain,
):
    sizes = {a: lax.axis_size(a) for a in ("dp_0", "dp_1", "dp_2", "dp_3", "tensor")}
    nz, nx, ny = sizes["dp_0"], sizes["dp_1"], sizes["dp_2"]
    seq, features = tokens.shape
    own_rows, cols = output_weight.shape
    gcols = inner_weight.shape[1]
    heads = step_weight.shape[1]
    chunks = features // CHUNK
    groups = gcols // HEAD_DIM
    f32, half = jnp.float32, jnp.bfloat16
    vmem = pl.BlockSpec(memory_space=pltpu.VMEM)
    dma = pltpu.SemaphoreType.DMA
    return pl.pallas_call(
        functools.partial(step_kernel, sizes),
        name="whole_step",
        out_shape=(
            jax.ShapeDtypeStruct((1, 128), f32),
            jax.ShapeDtypeStruct((own_rows, gcols), f32),
        ),
        in_specs=[pl.BlockSpec(memory_space=pl.ANY)] * 9,
        out_specs=(vmem,) * 2,
        scratch_shapes=[
            pltpu.VMEM((seq, features), half),
            pltpu.VMEM((seq, features), half),
            pltpu.VMEM((own_rows, gcols), f32),
            pltpu.VMEM((own_rows, cols), half),
            pltpu.VMEM((state_weight.shape[1], features), half),
            pltpu.VMEM((heads, features), half),
            pltpu.VMEM((1, heads), f32),
            pltpu.VMEM((1, heads), f32),
            pltpu.VMEM((1, heads), f32),
            dma((9,)),
            dma((2,)),
            dma((2,)),
            pltpu.VMEM((own_rows, gcols), half),
            pltpu.VMEM((nz, nx, ny, 2, own_rows, gcols), half),
            pltpu.VMEM((nz, nx, ny, 2, own_rows, cols), half),
            pltpu.VMEM((heads, seq, seq), half),
            pltpu.VMEM((groups, seq, heads // groups * seq), half),
            pltpu.VMEM((seq, cols), half),
            pltpu.VMEM((nz, nx, ny, 2, own_rows, seq), half),
            pltpu.VMEM((2 * nx, nz, ny, own_rows, seq), half),
            pltpu.VMEM((chunks, seq, CHUNK), f32),
            pltpu.VMEM((NARROW, seq, CHUNK), half),
            pltpu.VMEM((NARROW, seq, CHUNK), half),
            pltpu.VMEM((chunks - NARROW, seq, CHUNK), f32),
            pltpu.VMEM((seq, cols), f32),
            pltpu.VMEM((groups, 2 * nx, seq, HEAD_DIM), half),
            pltpu.VMEM((groups, nz, ny, own_rows, HEAD_DIM), f32),
            pltpu.VMEM((groups, nz, ny, own_rows, HEAD_DIM), half),
            pltpu.VMEM((groups, nz * ny, own_rows, HEAD_DIM), half),
            pltpu.VMEM((nx * ny * 4, 1, 128), f32),
            pltpu.VMEM((nz, 1, 128), f32),
            dma, dma((nz * nx * ny,)), dma, dma, dma((nz * nx * ny,)), dma((nz,)),
            dma((2,)), dma((chunks,)), dma, dma, dma, dma((groups, 2 * nx)),
            dma, dma((groups,)), dma, dma, dma, dma,
        ],
        compiler_params=pltpu.CompilerParams(
            collective_id=0, has_side_effects=True, vmem_limit_bytes=60 * 1024 * 1024
        ),
    )(
        tokens, teacher, inner_weight, output_weight, state_weight.T, step_weight.T,
        step_bias[None, :], decay_log[None, :], skip_gain[None, :],
    )


def on_device(
    tokens,
    teacher,
    inner_weight,
    output_weight,
    inner_first,
    inner_second,
    state_weight,
    step_weight,
    step_bias,
    decay_log,
    skip_gain,
):
    loss, clipped = whole_step(
        tokens, teacher, inner_weight, output_weight, state_weight, step_weight,
        step_bias, decay_log, skip_gain,
    )
    first_fix = 1.0 - beta_one**STEP
    second_fix = 1.0 - beta_two**STEP
    first_next = beta_one * inner_first + (1.0 - beta_one) * clipped
    second_next = beta_two * inner_second + (1.0 - beta_two) * clipped * clipped
    update = (
        first_next / first_fix / (jnp.sqrt(second_next / second_fix) + adam_eps)
        + weight_decay * inner_weight
    )
    return (loss[0, 0], update, first_next, second_next)


def solution(mesh):
    finer = Mesh(
        mesh.devices.reshape(8, 4, 2, 2, mesh.shape["tensor"]),
        ("dp_0", "dp_1", "dp_2", "dp_3", "tensor"),
    )
    return jax.shard_map(
        on_device,
        mesh=finer,
        in_specs=(
            P(DP, None),
            P(DP, None),
            P(DP, "tensor"),
            P(DP, "tensor"),
            P(DP, "tensor"),
            P(DP, "tensor"),
            P(),
            P(None, "tensor"),
            P("tensor"),
            P("tensor"),
            P("tensor"),
        ),
        out_specs=(P(), P(DP, "tensor"), P(DP, "tensor"), P(DP, "tensor")),
        check_vma=False,
    )
```

```python
import functools
import heapq

import jax
import jax.numpy as jnp
from jax import lax
from jax.experimental import pallas as pl
from jax.experimental.pallas import tpu as pltpu
from jax.sharding import Mesh
from jax.sharding import PartitionSpec as P

HEAD_DIM = 128
STEP = 20
DP = ("dp_0", "dp_1", "dp_2", "dp_3")


beta_one = 0.9
beta_two = 0.95
adam_eps = 1e-08
weight_decay = 0.1
norm_eps = 1e-06


TORUS = ("dp_0", "dp_1", "dp_2")
BY_COLUMN = (("dp_2", "dp_1", "dp_0"), 2, False)
BY_ROW = (("dp_0", "dp_2", "dp_1"), 1, True)
CHUNK = 256
NARROW = 3
MIX_AT = 9.0


def ways(sizes):
    def sign(rel, order):
        n, v = sizes[order[2]], rel[order[2]]
        if 2 * v == n:
            return 1 if (rel[order[0]] + rel[order[1]]) % 2 == 0 else -1
        return 1 if 2 * v < n else -1

    def onward(rel, order):
        last = order[2]
        n = sizes[last]
        if rel[last] == 0:
            moves = [1, -1] if n > 2 else [1]
        else:
            moves = [sign(rel, order)]
        out = []
        for move in moves:
            nxt = dict(rel)
            nxt[last] = (rel[last] + move) % n
            far = nxt[last] if move > 0 else n - nxt[last]
            was = rel[last] if move > 0 else (n - rel[last]) % n
            if nxt[last] and far == was + 1 and (n == 2 or sign(nxt, order) == move):
                out.append(nxt)
        return out

    def children(rel, tree):
        order, straight, jump = tree
        last = order[2]
        if jump:
            out = [{**rel, last: v} for v in range(1, sizes[last])] if rel[last] == 0 else []
        else:
            out = onward(rel, order)
        zero = {a: 0 for a in TORUS}
        if not any(rel.values()):
            for i in range(sizes[order[0]]):
                for j in range(sizes[order[1]] if straight == 2 else 1):
                    if i or j:
                        out.append({**zero, order[0]: i, order[1]: j})
        if straight == 1 and rel[order[1]] == 0 and rel[order[2]] == 0:
            out += [{**rel, order[1]: j} for j in range(1, sizes[order[1]])]
        out.sort(key=lambda r: -sum(min(v, sizes[a] - v) for a, v in r.items()))
        return out

    return children


def relay_times(sizes, flows, latency=2.6, hop=0.45):
    children = ways(sizes)
    free, heap, count = {}, [], 0
    events = [[] for _ in flows]
    for n, (order, wire, start) in enumerate(flows):
        heapq.heappush(heap, (start, count, n, {a: 0 for a in TORUS}))
        count += 1
    while heap:
        now, _, n, rel = heapq.heappop(heap)
        order, wire, _ = flows[n]
        sends = children(rel, order)
        events[n].append((now, rel, sends))
        for nxt in sends:
            lands, hops = now, 0
            for a in TORUS:
                v = (nxt[a] - rel[a]) % sizes[a]
                if v:
                    go = 1 if 2 * v <= sizes[a] else -1
                    far = min(v, sizes[a] - v) * (2 if sizes[a] == 2 else 1)
                    begin = max(now, free.get((a, go), 0.0))
                    free[(a, go)] = begin + wire * far
                    lands = max(lands, begin + wire)
                    hops += far
            heapq.heappush(heap, (lands + latency + hop * (hops - 1) + (1.0 if n % 2 == 0 else 0.0), count, n, nxt))
            count += 1
    return events


def step_kernel(
    sizes,
    tokens_hbm, teacher_hbm, inner_weight_hbm, output_weight_hbm, state_weight_hbm,
    step_weight_hbm, step_bias_hbm, decay_log_hbm, skip_hbm,
    loss_out, clipped_out,
    tokens, teacher, inner_weight, output_weight, state_weight,
    step_weight, step_bias, decay_log, skip, load_sem, lend_send, lend_recv,
    mine, in_all, w_all, mix, mix_t, inner,
    tok_t, tok_all, part, leaving, arrived, arrived_wide, grad_acc, gp_all, g_part, g_half, g_all, row_a, row_b,
    in_send, in_recv, in_pair, w_send, w_recv, w_pair,
    student_send, student_recv, tok_send, tok_recv, gp_send, gp_recv,
    g_send, g_recv, a_send, a_recv, b_send, b_recv,
):
    axes = ("dp_0", "dp_1", "dp_2", "dp_3", "tensor")
    here = {a: lax.axis_index(a) for a in axes}
    nz, nx, ny = sizes["dp_0"], sizes["dp_1"], sizes["dp_2"]
    seq, features = tokens.shape
    cols = output_weight.shape[1]
    chunks = features // CHUNK
    heads = mix.shape[0]
    head_dim = cols // heads
    groups = inner_weight.shape[1] // head_dim
    per_group = heads // groups
    core = here["dp_3"]

    def ahead(a, v):
        return lax.rem(here[a] + (v % sizes[a]), sizes[a])

    def there(**by):
        return {a: ahead(a, v) for a, v in by.items() if v % sizes[a]}

    def remote(src, dst, send, recv, target):
        return pltpu.make_async_remote_copy(
            src, dst, send, recv, device_id=target, device_id_type=pl.DeviceIdType.MESH
        )

    plane = [
        dict(dp_1=i, dp_2=j, dp_3=k, tensor=t)
        for i in range(nx) for j in range(ny) for k in range(2) for t in range(2)
    ][1:]
    column = [dict(dp_0=i, dp_2=j) for i in range(nz) for j in range(ny)][1:]
    peers = plane + [dict(dp_0=i) for i in range(1, nz)]
    pair = there(dp_3=1)
    loads = [
        pltpu.make_async_copy(source, target, load_sem.at[n])
        for n, (source, target) in enumerate((
            (inner_weight_hbm, inner_weight), (output_weight_hbm, output_weight),
            (state_weight_hbm, state_weight), (step_weight_hbm, step_weight),
            (step_bias_hbm, step_bias), (decay_log_hbm, decay_log), (skip_hbm, skip),
            (tokens_hbm, tokens), (teacher_hbm, teacher),
        ))
    ]
    borrows = jnp.logical_and(core == 1, here["tensor"] == 1)
    lends = jnp.logical_and(core == 1, here["tensor"] == 0)
    lent = [
        remote(ref, ref, lend_send.at[n], lend_recv.at[n], there(tensor=1, dp_2=1))
        for n, ref in enumerate((tokens, teacher))
    ]
    for load in loads[:-2]:
        load.start()

    @pl.when(jnp.logical_not(borrows))
    def _():
        for load in loads[-2:]:
            load.start()

    barrier = pltpu.get_barrier_semaphore()
    for by in peers:
        pl.semaphore_signal(
            barrier, inc=1, device_id=there(**by), device_id_type=pl.DeviceIdType.MESH
        )
    for load in loads[:2]:
        load.wait()
    mine[...] = inner_weight[...].astype(jnp.bfloat16)
    in_all[here["dp_0"], here["dp_1"], here["dp_2"], core] = mine[...]
    w_all[here["dp_0"], here["dp_1"], here["dp_2"], core] = output_weight[...]

    in_wire, w_wire = 0.088, 0.352
    flows = (
        (BY_ROW, in_wire, 0.0), (BY_ROW, in_wire, 0.0),
        (BY_COLUMN, w_wire, -0.01), (BY_COLUMN, w_wire, -0.01),
    )
    events = relay_times(sizes, flows)
    steps = [
        sorted(
            [(t, 0, rel, sends) for t, rel, sends in events[c]]
            + [(t, 1, rel, sends) for t, rel, sends in events[2 + c]],
            key=lambda e: e[:2],
        )
        for c in range(2)
    ]

    def number(rel):
        return (rel["dp_0"] * nx + rel["dp_1"]) * ny + rel["dp_2"]

    def relay(c, begin, end):
        for time, kind, rel, sends in steps[c]:
            if not begin <= time < end:
                continue
            all_ref, own, send, recv = (
                (in_all, mine, in_send, in_recv), (w_all, output_weight, w_send, w_recv)
            )[kind]
            at = tuple(ahead(a, -rel[a]) for a in TORUS)
            slot = all_ref.at[at[0], at[1], at[2], c]
            first = not any(rel.values())
            block = own if first else slot
            if not first:
                remote(slot, slot, send, recv.at[number(rel)], pair).wait_recv()
            for nxt in sends:
                target = there(**{a: nxt[a] - rel[a] for a in TORUS})
                remote(block, slot, send, recv.at[number(nxt)], target).start()
            beside = in_pair if kind == 0 else w_pair.at[rel["dp_0"]]
            remote(block, slot, send, beside, pair).start()

    def relay_until(begin, end):
        for c in range(2):
            @pl.when(core == c)
            def _():
                relay(c, begin, end)

    def turn_tokens():
        per = tok_t.shape[4]
        rows_x = ny * 2 * per
        for k in range(features // 128):
            turned = tokens[:, k * 128 : (k + 1) * 128].T
            z, x = divmod(k * 128 // rows_x, nx)
            tok_t[z, x : x + 128 // rows_x] = turned.reshape(128 // rows_x, ny, 2, per, seq)

    def mix_heads():
        projected = lax.dot_general(
            tokens[...], state_weight[...], (((1,), (1,)), ((), ())),
            preferred_element_type=jnp.float32,
        )
        width = projected.shape[1] // 2
        b_coef, c_coef = projected[:, :width], projected[:, width:]
        gram = lax.dot_general(
            c_coef, b_coef, (((1,), (1,)), ((), ())),
            precision=lax.Precision.HIGHEST, preferred_element_type=jnp.float32,
        )
        raw = (
            lax.dot_general(
                tokens[...], step_weight[...], (((1,), (1,)), ((), ())),
                preferred_element_type=jnp.float32,
            )
            + step_bias[...]
        )
        step_size = jnp.maximum(raw, 0.0) + jnp.log1p(jnp.exp(-jnp.abs(raw)))
        rate = jnp.exp(decay_log[...]) * step_size
        later = lax.broadcasted_iota(jnp.int32, (seq, seq), 0)
        earlier = lax.broadcasted_iota(jnp.int32, (seq, seq), 1)
        causal = later >= earlier
        cumulative = jnp.dot(
            causal.astype(jnp.float32), rate,
            precision=lax.Precision.HIGHEST, preferred_element_type=jnp.float32,
        )
        blank = jnp.zeros((seq, seq - heads), jnp.float32)
        cum_t = jnp.concatenate([cumulative, blank], axis=1).T
        step_t = jnp.concatenate([step_size, blank], axis=1).T
        for h in range(heads):
            log_decay = cum_t[h : h + 1, :] - cumulative[:, h : h + 1]
            decay = jnp.where(causal, jnp.exp(jnp.minimum(log_decay, 0.0)), 0.0)
            mix[h] = (gram * decay * step_t[h : h + 1, :]).astype(jnp.bfloat16)

    def turn_mix():
        for g in range(groups):
            for h in range(per_group):
                mix_t[g, :, h * seq : (h + 1) * seq] = mix[g * per_group + h].T

    def project():
        width = inner_weight.shape[1]
        projected = jnp.dot(
            tokens[...], in_all[...].reshape(features, width),
            preferred_element_type=jnp.float32,
        ).astype(jnp.bfloat16)
        for g in range(groups):
            source = projected[:, g * head_dim : (g + 1) * head_dim]
            stack = mix[g * per_group : (g + 1) * per_group].reshape(per_group * seq, seq)
            mixed = jnp.dot(stack, source, preferred_element_type=jnp.float32)
            wide = source.astype(jnp.float32)
            for h in range(per_group):
                n = g * per_group + h
                inner[:, n * head_dim : (n + 1) * head_dim] = (
                    mixed[h * seq : (h + 1) * seq] + skip[:, n : n + 1] * wide
                ).astype(jnp.bfloat16)

    other_half = {"tensor": 1 - here["tensor"], "dp_2": lax.rem(here["dp_2"] + core, ny)}
    order = sorted(range(nz), key=lambda v: (min(v, nz - v), v))

    wide = chunks - leaving.shape[0]

    def student_copy(i):
        source, target = (part, arrived_wide) if i < wide else (leaving, arrived)
        at = i if i < wide else i - wide
        return remote(
            source.at[at], target.at[at], student_send.at[int(i < wide)],
            student_recv.at[i], other_half,
        )

    def came(i):
        return arrived_wide[i] if i < wide else arrived[i - wide].astype(jnp.float32)

    def w_rows(i):
        return w_all[ahead("dp_0", -order[i])].reshape(CHUNK, cols)

    def teacher_cols(i):
        return teacher[:, pl.ds(pl.multiple_of(ahead("dp_0", -order[i]) * CHUNK, CHUNK), CHUNK)]

    def student(i):
        beside = w_all.at[0, :, :, 0]
        remote(beside, beside, w_send, w_pair.at[order[i]], pair).wait_recv()
        piece = lax.dot_general(
            inner[...], w_rows(i), (((1,), (1,)), ((), ())), preferred_element_type=jnp.float32
        )
        part[i] = piece
        if i >= wide:
            leaving[i - wide] = piece.astype(jnp.bfloat16)
        if i:
            student_copy(i - 1).start()

    pl.semaphore_wait(barrier, len(peers))
    late = max(t for t, *_ in steps[0] + steps[1]) + 1
    inner_done = max(t for c in range(2) for t, kind, *_ in steps[c] if kind == 0) + 1e-6
    @pl.when(jnp.logical_not(borrows))
    def _():
        for load in loads[-2:]:
            load.wait()

    @pl.when(lends)
    def _():
        for copy in lent:
            copy.start()

    relay_until(-1.0, 2.0)
    for load in loads[2:-2]:
        load.wait()
    relay_until(2.0, MIX_AT)

    @pl.when(borrows)
    def _():
        lent[0].wait_recv()

    turn_tokens()
    mix_heads()
    turn_mix()
    relay_until(MIX_AT, max(inner_done, MIX_AT))
    beside = in_all.at[:, :, :, 0]
    remote(beside, beside, in_send, in_pair, pair).wait_recv()
    project()
    tok_sends = []
    for i in range(nx):
        for k in range(2):
            slot = i * 2 + k
            to_x = lax.rem(here["dp_1"] + i, nx)
            to_c = lax.rem(here["dp_3"] + k, 2)
            if slot:
                tok_sends.append((slot, to_x, to_c, there(dp_1=i, dp_3=k)))
    for slot, to_x, to_c, target in tok_sends:
        remote(
            tok_t.at[:, to_x, :, to_c], tok_all.at[slot], tok_send, tok_recv, target
        ).start()
    tok_all[0] = tok_t[:, here["dp_1"], :, here["dp_3"]]

    reached = max(inner_done, MIX_AT)
    for i in range(chunks):
        needed = max(
            t for c in range(2) for t, kind, rel, _ in steps[c]
            if kind == 1 and rel["dp_0"] == order[i]
        ) + 1e-6
        if needed > reached:
            relay_until(reached, needed)
            reached = needed
        student(i)
    relay_until(reached, late)
    student_copy(chunks - 1).start()

    @pl.when(borrows)
    def _():
        lent[1].wait_recv()

    @pl.when(lends)
    def _():
        for copy in lent:
            copy.wait_send()

    squares = jnp.zeros((8, CHUNK), jnp.float32)
    for i in range(chunks):
        student_copy(i).wait_recv()
        error = (
            part[i] + came(i)
            - teacher_cols(i).astype(jnp.float32)
        )
        squares = squares + jnp.sum((error * error).reshape(seq // 8, 8, CHUNK), axis=0)
        product = jnp.dot(
            error.astype(jnp.bfloat16), w_rows(i), preferred_element_type=jnp.float32,
        )
        if i == 0:
            grad_acc[...] = product
        else:
            grad_acc[...] += product
    near = (1, 3, 2) if nx == 4 else range(1, nx)
    members = 2 * nx

    def gp_copy(g, source, slot, target):
        return remote(
            gp_all.at[g, source], gp_all.at[g, slot], gp_send, gp_recv.at[g, slot], target
        )

    for g in range(groups):
        heads_here = []
        direct = None
        for h in range(per_group):
            n = g * per_group + h
            one = grad_acc[:, n * head_dim : (n + 1) * head_dim].astype(jnp.bfloat16)
            heads_here.append(one)
            term = skip[:, n : n + 1] * one.astype(jnp.float32)
            direct = term if direct is None else direct + term
        back = jnp.dot(
            mix_t[g], jnp.concatenate(heads_here, axis=0), preferred_element_type=jnp.float32
        )
        gp_all[g, 0] = (back + direct).astype(jnp.bfloat16)
        for i in reversed(near):
            gp_copy(g, 0, 2 * i, there(dp_1=i)).start()
        gp_copy(g, 0, 1, pair).start()
    remote(
        tok_all.at[pl.ds(1, members - 1)], tok_all.at[pl.ds(1, members - 1)],
        tok_send, tok_recv, pair,
    ).wait()

    def product_of(g, slot):
        left = tok_all[slot].reshape(-1, seq)
        return jnp.dot(left, gp_all[g, slot], preferred_element_type=jnp.float32)

    outward = sorted(column, key=lambda b: -min(b["dp_0"], nz - b["dp_0"]) - b["dp_2"])
    for g in range(groups):
        gp_copy(g, 1, 1, pair).wait_recv()
        total = product_of(g, 0) + product_of(g, 1)
        for i in near:
            gp_copy(g, 0, 2 * i, pair).wait_recv()
            gp_copy(g, 2 * i, 2 * i + 1, pair).start()
            total = total + product_of(g, 2 * i)
        for i in near:
            gp_copy(g, 0, 2 * i + 1, pair).wait_recv()
            total = total + product_of(g, 2 * i + 1)
        g_half[g] = total.reshape(g_part.shape[1:]).astype(jnp.bfloat16)
        g_part[g] = total.reshape(g_part.shape[1:])
        for by in outward:
            slot = by["dp_0"] * ny + by["dp_2"]
            to_z, to_y = ahead("dp_0", by["dp_0"]), ahead("dp_2", by["dp_2"])
            remote(
                g_half.at[g, to_z, to_y], g_all.at[g, slot], g_send, g_recv.at[g], there(**by)
            ).start()
    err = jnp.sum(squares) * 0.5
    halves = []
    for g in range(groups):
        rest = g_all.at[g, pl.ds(1, nz * ny - 1)]
        remote(rest, rest, g_send, g_recv.at[g], pair).wait_recv()
        halves.append(
            g_part[g, here["dp_0"], here["dp_2"]]
            + jnp.sum(g_all[g, 1:].astype(jnp.float32), axis=0)
        )
    grad = jnp.concatenate(halves, axis=1)
    lane = lax.broadcasted_iota(jnp.int32, (1, 128), 1)
    row = jnp.where(lane == 0, jnp.sum(grad * grad), jnp.where(lane == 1, err, 0.0))
    row_a[0] = row
    for n, by in enumerate(plane):
        remote(row_a.at[0], row_a.at[n + 1], a_send, a_recv, there(**by)).start()
    rest = row_a.at[pl.ds(1, len(plane))]
    remote(rest, rest, a_send, a_recv, pair).wait()
    row_b[0] = jnp.sum(row_a[...], axis=0)
    for i in range(1, nz):
        remote(row_b.at[0], row_b.at[i], b_send, b_recv, there(dp_0=i)).start()
    rest = row_b.at[pl.ds(1, nz - 1)]
    remote(rest, rest, b_send, b_recv, pair).wait()
    sums = jnp.sum(row_b[...], axis=0)
    root_mean = jnp.sqrt(sums[:, 0:1] / (features * inner_weight.shape[1] * 2))
    factor = jnp.minimum(1.0, 1.0 / (root_mean + norm_eps))
    loss_out[0, 0] = jnp.sum(jnp.where(lane == 1, sums, 0.0)) / (nz * nx * ny * 2 * seq * features)
    clipped_out[...] = factor * grad
    for g in range(groups):
        rest = gp_all.at[g, pl.ds(1, members - 1)]
        remote(rest, rest, gp_send, gp_recv.at[g, 1], pair).wait_send()
        rest = g_all.at[g, pl.ds(1, nz * ny - 1)]
        remote(rest, rest, g_send, g_recv.at[g], pair).wait_send()
    remote(leaving, leaving, student_send.at[0], student_recv.at[0], pair).wait_send()
    remote(arrived_wide, arrived_wide, student_send.at[1], student_recv.at[0], pair).wait_send()
    pieces = nz * nx * ny
    for block, ref, send in (((0,), in_all, in_send), ((0,), w_all, w_send)):
        half = ref.at[:, :, :, 0]
        remote(half, half, send, in_pair, pair).wait_send()
        rest = ref.at[pl.ds(0, nz - 1), :, :, 0]
        remote(rest, rest, send, in_pair, pair).wait_send()
        rest = ref.at[0, pl.ds(0, nx - 1), :, 0]
        remote(rest, rest, send, in_pair, pair).wait_send()
        rest = ref.at[0, 0, pl.ds(0, ny - 1), 0]
        remote(rest, rest, send, in_pair, pair).wait_send()


def whole_step(
    tokens, teacher, inner_weight, output_weight, state_weight, step_weight,
    step_bias, decay_log, skip_gain,
):
    sizes = {a: lax.axis_size(a) for a in ("dp_0", "dp_1", "dp_2", "dp_3", "tensor")}
    nz, nx, ny = sizes["dp_0"], sizes["dp_1"], sizes["dp_2"]
    seq, features = tokens.shape
    own_rows, cols = output_weight.shape
    gcols = inner_weight.shape[1]
    heads = step_weight.shape[1]
    chunks = features // CHUNK
    groups = gcols // HEAD_DIM
    f32, half = jnp.float32, jnp.bfloat16
    vmem = pl.BlockSpec(memory_space=pltpu.VMEM)
    dma = pltpu.SemaphoreType.DMA
    return pl.pallas_call(
        functools.partial(step_kernel, sizes),
        name="whole_step",
        out_shape=(
            jax.ShapeDtypeStruct((1, 1), f32),
            jax.ShapeDtypeStruct((own_rows, gcols), f32),
        ),
        in_specs=[pl.BlockSpec(memory_space=pl.ANY)] * 9,
        out_specs=(pl.BlockSpec(memory_space=pltpu.SMEM), vmem),
        scratch_shapes=[
            pltpu.VMEM((seq, features), half),
            pltpu.VMEM((seq, features), half),
            pltpu.VMEM((own_rows, gcols), f32),
            pltpu.VMEM((own_rows, cols), half),
            pltpu.VMEM((state_weight.shape[1], features), half),
            pltpu.VMEM((heads, features), half),
            pltpu.VMEM((1, heads), f32),
            pltpu.VMEM((1, heads), f32),
            pltpu.VMEM((1, heads), f32),
            dma((9,)),
            dma((2,)),
            dma((2,)),
            pltpu.VMEM((own_rows, gcols), half),
            pltpu.VMEM((nz, nx, ny, 2, own_rows, gcols), half),
            pltpu.VMEM((nz, nx, ny, 2, own_rows, cols), half),
            pltpu.VMEM((heads, seq, seq), half),
            pltpu.VMEM((groups, seq, heads // groups * seq), half),
            pltpu.VMEM((seq, cols), half),
            pltpu.VMEM((nz, nx, ny, 2, own_rows, seq), half),
            pltpu.VMEM((2 * nx, nz, ny, own_rows, seq), half),
            pltpu.VMEM((chunks, seq, CHUNK), f32),
            pltpu.VMEM((NARROW, seq, CHUNK), half),
            pltpu.VMEM((NARROW, seq, CHUNK), half),
            pltpu.VMEM((chunks - NARROW, seq, CHUNK), f32),
            pltpu.VMEM((seq, cols), f32),
            pltpu.VMEM((groups, 2 * nx, seq, HEAD_DIM), half),
            pltpu.VMEM((groups, nz, ny, own_rows, HEAD_DIM), f32),
            pltpu.VMEM((groups, nz, ny, own_rows, HEAD_DIM), half),
            pltpu.VMEM((groups, nz * ny, own_rows, HEAD_DIM), half),
            pltpu.VMEM((nx * ny * 4, 1, 128), f32),
            pltpu.VMEM((nz, 1, 128), f32),
            dma, dma((nz * nx * ny,)), dma, dma, dma((nz * nx * ny,)), dma((nz,)),
            dma((2,)), dma((chunks,)), dma, dma, dma, dma((groups, 2 * nx)),
            dma, dma((groups,)), dma, dma, dma, dma,
        ],
        compiler_params=pltpu.CompilerParams(
            collective_id=0, has_side_effects=True, vmem_limit_bytes=60 * 1024 * 1024
        ),
    )(
        tokens, teacher, inner_weight, output_weight, state_weight.T, step_weight.T,
        step_bias[None, :], decay_log[None, :], skip_gain[None, :],
    )


def on_device(
    tokens,
    teacher,
    inner_weight,
    output_weight,
    inner_first,
    inner_second,
    state_weight,
    step_weight,
    step_bias,
    decay_log,
    skip_gain,
):
    loss, clipped = whole_step(
        tokens, teacher, inner_weight, output_weight, state_weight, step_weight,
        step_bias, decay_log, skip_gain,
    )
    first_fix = 1.0 - beta_one**STEP
    second_fix = 1.0 - beta_two**STEP
    first_next = beta_one * inner_first + (1.0 - beta_one) * clipped
    second_next = beta_two * inner_second + (1.0 - beta_two) * clipped * clipped
    update = (
        first_next / first_fix / (jnp.sqrt(second_next / second_fix) + adam_eps)
        + weight_decay * inner_weight
    )
    return (loss[0, 0], update, first_next, second_next)


def solution(mesh):
    finer = Mesh(
        mesh.devices.reshape(8, 4, 2, 2, mesh.shape["tensor"]),
        ("dp_0", "dp_1", "dp_2", "dp_3", "tensor"),
    )
    return jax.shard_map(
        on_device,
        mesh=finer,
        in_specs=(
            P(DP, None),
            P(DP, None),
            P(DP, "tensor"),
            P(DP, "tensor"),
            P(DP, "tensor"),
            P(DP, "tensor"),
            P(),
            P(None, "tensor"),
            P("tensor"),
            P("tensor"),
            P("tensor"),
        ),
        out_specs=(P(), P(DP, "tensor"), P(DP, "tensor"), P(DP, "tensor")),
        check_vma=False,
    )
```
